32 devices in a mesh: task: 16 (over z, x, core), tensor: 2 (over y).
Axes of the slice: x: 2, y: 2, z: 4, core: 2. Of those that a mesh axis runs over, the one named last changes fastest.
Arguments:
- inputs: bfloat16 [2048, 4096], P('task', 'tensor'), may hold values from -6 to 6
- targets: bfloat16 [2048, 4096], P('task', 'tensor'), may hold values from -6 to 6
- queries: bfloat16 [2048, 2048], P('task', 'tensor'), may hold values from -120 to 120
- key_rows: bfloat16 [2048, 2048], P('task', 'tensor'), may hold values from -4 to 4
- value_weight: bfloat16 [4096, 2048], P(None, 'tensor'), may hold values from -0.09375 to 0.09375
- output_weight: bfloat16 [2048, 4096], P('tensor'), may hold values from -0.125 to 0.125
- splits: int32 [16], P('task'), may hold values from 32 to 96
Outputs:
- meta_value: float32 [4096, 2048], P('task', 'tensor')
- meta_output: float32 [2048, 4096], P('tensor', 'task')
The draws below stay inside these ranges and needn't reach their ends.
Inputs may be any that keep to these rules, and one draw needn't show every extreme that they name: `splits`: support and query parts of every task are both nonempty.
All inputs are finite; a program needn't handle non-finite values.
Results may differ from the reference program's by a relative error of at most 0.025.
Values may be sent and summed in bfloat16 or wider, within the bound.
No kernel may reach another device: no remote copies, remote signals or barrier semaphores. Data moves between devices by JAX's collectives and lax.ppermute only.
A program may use at most 128 MiB of HBM per device.

```python
import jax
import jax.numpy as jnp
from jax import lax

D = 4096
HD = 128
HEADS = 16
INNER = 1
TASKS_DEV = 1
TASK_LEN = 128
TOKENS = 2048
N_TASK = 16
N_TENSOR = 2


def paired(key):
    first, second = jax.random.split(jax.random.fold_in(key, 7), 2)
    query_base = jnp.clip(jax.random.normal(first, (TOKENS, HEADS * HD), jnp.float32), -4.0, 4.0)
    key_base = jnp.clip(jax.random.normal(second, (TOKENS, HEADS * HD), jnp.float32), -4.0, 4.0)
    return (query_base, key_base)


def draw_queries(key, part):
    return paired(key)[0].astype(jnp.bfloat16)


def draw_key_rows(key, part):
    return paired(key)[1].astype(jnp.bfloat16)


def touch_ends(values, own_key, smallest, high):
    extent = values.shape
    place = [jax.random.randint(jax.random.fold_in(own_key, axis), (), 0, extent[axis]) for axis in range(len(extent))]
    values = values.at[tuple(place)].set(smallest)
    longest = extent.index(max(extent))
    place[longest] = (place[longest] + 1) % extent[longest]
    return values.at[tuple(place)].set(high)


def spiked(drawn, stream_key, source, target, blocks, factor):
    def block_of(dim):
        return (jnp.arange(drawn.shape[dim]) // (drawn.shape[dim] // blocks)).reshape((-1,) + (1,) * (drawn.ndim - 1 - dim))

    one_side = jax.random.permutation(stream_key, blocks)[block_of(target)]
    second = (block_of(target) + blocks // 2) % blocks
    return jnp.where((block_of(source) == one_side) | (block_of(source) == second), factor * drawn, drawn)


def steps_of(own_key, shape, cuts, low, top_value):
    level, own = 1.0, jax.random.fold_in(own_key, 6)
    for dim, blocks in cuts:
        heights = jnp.exp(jax.random.uniform(jax.random.fold_in(own, dim), (blocks,), jnp.float32, low / len(cuts), top_value / len(cuts)))
        level = level * jnp.repeat(heights, shape[dim] // blocks).reshape([-1 if axis == dim else 1 for axis in range(len(shape))])
    return level


def bell_draw(own_key, extent, scale, reach, pieces=(), kind=jnp.bfloat16):
    array = jax.random.normal(own_key, extent, jnp.float32) * scale
    if len(pieces) > 0:
        array = steps_of(own_key, extent, pieces, -0.22, 0.18) * array
    return jnp.clip(array, min=-reach, max=reach).astype(kind)


def gaussian_with(stream_key, shape, scale, most, shards, heavy, held_as=jnp.bfloat16):
    entries = scale * jax.random.normal(stream_key, shape, jnp.float32)
    if shards:
        entries = entries * steps_of(stream_key, shape, shards, -0.22, 0.18)
    return jnp.clip(spiked(entries, jax.random.fold_in(stream_key, 3), *heavy), -most, most).astype(held_as)


def setup_inputs(seed: int = 0) -> dict:
    streams_of = jax.random.split(jax.random.key(seed), 8)
    return {
        "inputs": gaussian_with(streams_of[0], (TOKENS, D), 1.0, 6.0, ((0, 16), (1, 2)), (0, 1, 16, 2.0)),
        "targets": bell_draw(streams_of[1], (TOKENS, D), 1.0, 6.0, ((0, 16), (1, 2))),
        "queries": draw_queries(jax.random.fold_in(streams_of[7], 71), 0),
        "key_rows": draw_key_rows(jax.random.fold_in(streams_of[7], 71), 0),
        "value_weight": bell_draw(streams_of[4], (D, HEADS * HD), D ** -0.5, 0.09375, ((1, 2),)),
        "output_weight": bell_draw(streams_of[5], (HEADS * HD, D), (HEADS * HD) ** -0.5, 0.125, ((0, 2),)),
        "splits": touch_ends(jax.random.randint(streams_of[6], (TASKS_DEV * N_TASK,), TASK_LEN // 4, 3 * TASK_LEN // 4 + 1), jax.random.fold_in(streams_of[6], 1), TASK_LEN // 4, (3 * TASK_LEN // 4 + 1) - 1).astype(jnp.int32),
    }


step_rate = 0.25

def normed_rows(inputs):
    values = inputs.astype(jnp.float32)
    scale = lax.rsqrt(lax.optimization_barrier(jnp.mean(values * values, axis=-1, keepdims=True)) + 1e-05)
    return (values * scale).astype(jnp.bfloat16)

def attention_probs(queries, key_rows, heads):
    length = queries.shape[0]
    query_f = queries.astype(jnp.float32).reshape(length, heads, -1)
    key_f = key_rows.astype(jnp.float32).reshape(length, heads, -1)
    scores = jnp.einsum('ihd,jhd->hij', query_f, key_f) / jnp.sqrt(jnp.float32(query_f.shape[2]))
    position = jnp.arange(length)
    causal = position[:, None] >= position[None, :]
    scores = jnp.where(causal[None], scores, jnp.float32(-1e+30))
    scores = scores - lax.optimization_barrier(jnp.max(scores, axis=-1, keepdims=True))
    expo = jnp.exp(scores)
    return (expo / lax.optimization_barrier(jnp.sum(expo, axis=-1, keepdims=True))).astype(jnp.bfloat16)

def local_out(value_mat, output_mat, normed, probs):
    heads = probs.shape[0]
    length = normed.shape[0]
    upper = jnp.dot(normed, value_mat.astype(jnp.bfloat16), preferred_element_type=jnp.float32).astype(jnp.bfloat16)
    mixed = jnp.einsum('hij,jhd->ihd', probs.astype(jnp.float32), upper.astype(jnp.float32).reshape(length, heads, -1))
    mixed = mixed.reshape(length, -1).astype(jnp.bfloat16)
    return jnp.dot(mixed, output_mat.astype(jnp.bfloat16), preferred_element_type=jnp.float32).astype(jnp.bfloat16)

def task_meta(value_mat, output_mat, inputs, targets, queries, key_rows, split):
    cols = HEADS * HD // N_TENSOR
    group = HEADS // N_TENSOR
    normed = normed_rows(inputs)
    probs = attention_probs(queries, key_rows, HEADS)
    position = jnp.arange(TASK_LEN)
    support = (position < split).astype(jnp.float32)[:, None]
    query_mask = 1.0 - support
    count_s = split.astype(jnp.float32)
    count_q = jnp.float32(TASK_LEN) - count_s
    input_f = inputs.astype(jnp.float32)
    target_f = targets.astype(jnp.float32)

    def total(value_now, output_now):
        result = input_f
        for index in range(N_TENSOR):
            result = result + local_out(value_now[:, index * cols:(index + 1) * cols], output_now[index * cols:(index + 1) * cols], normed, probs[index * group:(index + 1) * group]).astype(jnp.float32)
        return result

    def loss(value_now, output_now, mask, count):
        error = total(value_now, output_now) - target_f
        return 0.5 * jnp.sum(mask * error * error) / count

    def meta_loss(value_now, output_now):
        for inner in range(INNER):
            grad_value, grad_output = jax.grad(loss, argnums=(0, 1))(value_now, output_now, support, count_s)
            value_now = value_now - step_rate * grad_value
            output_now = output_now - step_rate * grad_output
        return loss(value_now, output_now, query_mask, count_q)
    return jax.grad(meta_loss, argnums=(0, 1))(value_mat, output_mat)

def reference(inputs, targets, queries, key_rows, value_weight, output_weight, splits):
    count = N_TASK * TASKS_DEV
    value_f = value_weight.astype(jnp.float32)
    output_f = output_weight.astype(jnp.float32)
    items = (inputs.reshape(count, TASK_LEN, D), targets.reshape(count, TASK_LEN, D), queries.reshape(count, TASK_LEN, HEADS * HD), key_rows.reshape(count, TASK_LEN, HEADS * HD), splits.astype(jnp.int32))

    def accumulate(carry, item):
        grad_value, grad_output = task_meta(value_f, output_f, item[0], item[1], item[2], item[3], item[4])
        return ((carry[0] + grad_value, carry[1] + grad_output), None)
    start = (jnp.zeros((D, HEADS * HD), jnp.float32), jnp.zeros((HEADS * HD, D), jnp.float32))
    result, unused = lax.scan(accumulate, start, items)
    return (result[0], result[1])
```

```python
import functools

import jax
import jax.numpy as jnp
from jax import lax
from jax.experimental import pallas as pl
from jax.experimental.pallas import tpu as pltpu
from jax.sharding import PartitionSpec as P

HD = 128
RATE = 0.25
CHUNKS = 4


f32 = jnp.float32
bf16 = jnp.bfloat16


def dot_nn(a, b):
    return lax.dot_general(a, b, (((1,), (0,)), ((), ())), preferred_element_type=f32)


def dot_nt(a, b):
    return lax.dot_general(a, b, (((1,), (1,)), ((), ())), preferred_element_type=f32)


def dot_tn(a, b):
    return lax.dot_general(a, b, (((0,), (0,)), ((), ())), preferred_element_type=f32)


def split_dot(dot, small, big):
    high = small.astype(bf16)
    low = (small - high.astype(f32)).astype(bf16)
    return dot(high, big) + dot(low, big)


def by_head(dot, probs_ref, value):
    heads = probs_ref.shape[0]
    rows = value.shape[0]
    return jnp.concatenate(
        [
            dot(probs_ref[h], value[:, h * HD : (h + 1) * HD])
            for h in range(heads)
        ],
        axis=1,
    )


def probs_kernel(query_ref, key_ref, out_ref):
    heads, length, unused = out_ref.shape
    row = lax.broadcasted_iota(jnp.int32, (length, length), 0)
    col = lax.broadcasted_iota(jnp.int32, (length, length), 1)
    for h in range(heads):
        cols = slice(h * HD, (h + 1) * HD)
        scores = dot_nt(query_ref[:, cols], key_ref[:, cols]) / jnp.sqrt(f32(HD))
        scores = jnp.where(row >= col, scores, f32(-1e30))
        expo = jnp.exp(scores - jnp.max(scores, axis=-1, keepdims=True))
        out_ref[h] = (expo / jnp.sum(expo, axis=-1, keepdims=True)).astype(bf16)


def first_kernel(x_ref, weight_ref, probs_ref, normed_ref, gram_ref, upper_ref, mixed_ref, keep_ref):
    @pl.when(pl.program_id(0) == 0)
    def _():
        values = x_ref[...].astype(f32)
        scale = lax.rsqrt(jnp.mean(values * values, axis=-1, keepdims=True) + 1e-05)
        normed = (values * scale).astype(bf16)
        keep_ref[...] = normed
        normed_ref[...] = normed
        gram_ref[...] = dot_nt(normed, normed)

    upper = dot_nn(keep_ref[...], weight_ref[...]).astype(bf16)
    upper_ref[...] = upper
    mixed_ref[...] = by_head(dot_nn, probs_ref, upper).astype(bf16)


def step_kernel(low, high, acc_ref, probs_ref, gram_ref, upper_ref, mixed_ref, next_ref, cross_high_ref, cross_low_ref):
    length, width = upper_ref.shape
    grad_mixed = jnp.sum(acc_ref[...], axis=0).astype(bf16)
    grad_mixed = jnp.concatenate([grad_mixed, jnp.zeros((length - high, width), bf16)], axis=0)
    grad_upper = by_head(dot_tn, probs_ref, grad_mixed).astype(bf16)
    upper = upper_ref[...].astype(f32) - RATE * split_dot(dot_nn, gram_ref[...], grad_upper)
    mixed_next = by_head(dot_nn, probs_ref, upper.astype(bf16)).astype(bf16)
    next_ref[...] = mixed_next
    cross = -RATE * dot_nt(mixed_next[low:], mixed_ref[:high])
    cross_high = cross.astype(bf16)
    cross_high_ref[...] = cross_high
    cross_low_ref[...] = (cross - cross_high.astype(f32)).astype(bf16)


def second_kernel(low, high, acc_ref, match_ref, probs_ref, gram_ref, mixed_ref, next_ref, tangent_ref, grad_ref):
    length, width = mixed_ref.shape
    match = -RATE * jnp.sum(match_ref[...], axis=0)
    grad_next = jnp.sum(acc_ref[...], axis=0) + split_dot(dot_nn, match, mixed_ref[:high])
    grad_next = jnp.concatenate([jnp.zeros((low, width), f32), grad_next], axis=0)
    grad_upper = by_head(dot_tn, probs_ref, grad_next.astype(bf16)).astype(bf16)
    upper_dot = -RATE * split_dot(dot_nn, gram_ref[...], grad_upper)
    tangent_ref[...] = by_head(dot_nn, probs_ref, upper_dot.astype(bf16)).astype(bf16)
    back = split_dot(dot_tn, match, next_ref[low:])
    back = jnp.concatenate([back, jnp.zeros((length - high, width), f32)], axis=0)
    grad_ref[...] = grad_next + back


def third_kernel(high, acc_ref, grad_ref, probs_ref, out_ref):
    length, width = grad_ref.shape
    extra = jnp.sum(acc_ref[...], axis=0)
    extra = jnp.concatenate([extra, jnp.zeros((length - high, width), f32)], axis=0)
    out_ref[...] = by_head(dot_tn, probs_ref, (grad_ref[...] + extra).astype(bf16)).astype(bf16)


def run(kernel, outs, *args):
    return pl.pallas_call(kernel, out_shape=outs)(*args)


def shape_of(shape, kind):
    return jax.ShapeDtypeStruct(shape, kind)


def per_device(n_task, n_tensor, inputs, targets, queries, key_rows, value_weight, output_weight, splits):
    length, part_width = inputs.shape
    wide = part_width * n_tensor
    heads = queries.shape[1] // HD
    width = heads * HD
    low, high = length // 4, length - length // 4
    lane = wide // CHUNKS
    group = lax.axis_index("tensor")
    task = lax.axis_index("task")
    split = splits[0]

    def over_tensor(value, shift):
        return lax.ppermute(value, "tensor", [(i, (i + shift) % n_tensor) for i in range(n_tensor)])

    def joined(value):
        whole = jnp.zeros((length, wide), value.dtype)
        for shift in range(n_tensor):
            piece = over_tensor(value, shift) if shift else value
            place = (group + (n_tensor - shift)) % n_tensor
            whole = lax.dynamic_update_slice(whole, piece, (0, place * part_width))
        return whole

    def summed(value):
        total = value.astype(f32)
        for shift in range(1, n_tensor):
            total = total + over_tensor(value, shift).astype(f32)
        return total

    def over_task(value, target):
        return lax.ppermute(value, "task", [(i, target(i)) for i in range(n_task)])

    def gathered(value):
        rows = value.shape[0]
        cores = 2 if n_task % 2 == 0 else 1
        pairs = 2 if n_task % (2 * cores) == 0 else 1
        inner = cores * pairs
        planes = n_task // inner
        blocks = []
        for turn in range(planes):
            def shifted(i, turn=turn):
                return ((i // inner + turn) % planes) * inner + i % inner
            piece = over_task(value, shifted) if turn else value
            plane = (task // inner + (planes - turn)) % planes
            blocks.append((piece, plane * inner + task % inner))
        if pairs == 2:
            blocks += [(over_task(b, lambda i: i ^ cores), m ^ cores) for b, m in blocks]
        if cores == 2:
            blocks += [(over_task(b, lambda i: i ^ 1), m ^ 1) for b, m in blocks]
        whole = jnp.zeros((n_task * rows, value.shape[1]), value.dtype)
        for block, source in blocks:
            whole = lax.dynamic_update_slice(whole, block, (source * rows, 0))
        return whole

    def spread(value):
        return lax.all_to_all(value, "task", split_axis=1, concat_axis=0, tiled=True)

    def cut(value, c):
        return value[:, c * lane : (c + 1) * lane]

    position = jnp.arange(length)
    count = split.astype(f32)
    in_support = (position < split)[:, None]
    support_weight = jnp.where(in_support, 1.0 / count, 0.0)
    query_weight = jnp.where(in_support, 0.0, 1.0 / (f32(length) - count))

    x_all = joined(inputs)
    t_all = joined(targets)
    probs = run(probs_kernel, shape_of((heads, length, length), bf16), queries, key_rows)

    block = 2 * HD if heads % 2 == 0 else HD
    normed, gram, upper, mixed = pl.pallas_call(
        first_kernel,
        grid=(width // block,),
        in_specs=[
            pl.BlockSpec((length, wide), lambda i: (0, 0)),
            pl.BlockSpec((wide, block), lambda i: (0, i)),
            pl.BlockSpec((block // HD, length, length), lambda i: (i, 0, 0)),
        ],
        out_specs=[
            pl.BlockSpec((length, wide), lambda i: (0, 0)),
            pl.BlockSpec((length, length), lambda i: (0, 0)),
            pl.BlockSpec((length, block), lambda i: (0, i)),
            pl.BlockSpec((length, block), lambda i: (0, i)),
        ],
        out_shape=[
            shape_of((length, wide), bf16),
            shape_of((length, length), f32),
            shape_of((length, width), bf16),
            shape_of((length, width), bf16),
        ],
        scratch_shapes=[pltpu.VMEM((length, wide), bf16)],
    )(x_all, value_weight, probs)
    normed_cols = spread(normed)

    offset = x_all.astype(f32) - t_all.astype(f32)
    mixed_s = mixed[:high]
    error_0 = []
    acc = []
    for c in range(CHUNKS):
        part = dot_nn(mixed_s, cut(output_weight, c)).astype(bf16)
        error = (support_weight[:high] * (cut(offset, c)[:high] + summed(part))).astype(bf16)
        error_0.append(error)
        acc.append(dot_nt(error, cut(output_weight, c)))
    error_0_cols = spread(jnp.concatenate(error_0, axis=1))

    rows = high
    mixed_next, cross_high, cross_low = run(
        functools.partial(step_kernel, low, high),
        [shape_of((length, width), bf16), shape_of((length - low, high), bf16), shape_of((length - low, high), bf16)],
        jnp.stack(acc), probs, gram, upper, mixed,
    )
    left_one = jnp.where(in_support, mixed, mixed_next)
    left_one_all = gathered(left_one)

    next_q = mixed_next[low:]
    error_q = []
    acc = []
    match = []
    for c in range(CHUNKS):
        part = dot_nn(next_q, cut(output_weight, c)) + (
            dot_nn(cross_high, error_0[c]) + dot_nn(cross_low, error_0[c])
        )
        part = part.astype(bf16)
        error = (query_weight[low:] * (cut(offset, c)[low:] + summed(part))).astype(bf16)
        error_q.append(error)
        acc.append(dot_nt(error, cut(output_weight, c)))
        match.append(dot_nt(error, error_0[c]))

    tangent, grad_rest = run(
        functools.partial(second_kernel, low, high),
        [shape_of((length, width), bf16), shape_of((length, width), f32)],
        jnp.stack(acc), jnp.stack(match), probs, gram, mixed, mixed_next,
    )
    tangent_s = tangent[:high]
    tangent_all = gathered(tangent_s)

    acc = []
    merged = []
    for c in range(CHUNKS):
        part = dot_nn(tangent_s, cut(output_weight, c)) + (
            dot_tn(cross_high, error_q[c]) + dot_tn(cross_low, error_q[c])
        )
        part = part.astype(bf16)
        back = (support_weight[:high] * summed(part)).astype(bf16)
        acc.append(dot_nt(back, cut(output_weight, c)))
        back_all = jnp.concatenate([back, jnp.zeros((length - high, lane), bf16)], axis=0)
        error_all = jnp.concatenate([jnp.zeros((low, lane), bf16), error_q[c]], axis=0)
        merged.append(jnp.where(in_support, back_all, error_all))
    merged_cols = spread(jnp.concatenate(merged, axis=1))

    right = run(
        functools.partial(third_kernel, high),
        shape_of((length, width), bf16),
        jnp.stack(acc), grad_rest, probs,
    )
    right_all = gathered(right)

    total_value = dot_tn(normed_cols, right_all)
    total_output = dot_tn(left_one_all, merged_cols) + dot_tn(tangent_all, error_0_cols)
    return (total_value, total_output)


def solution(mesh):
    body = functools.partial(per_device, mesh.shape["task"], mesh.shape["tensor"])
    return jax.shard_map(
        body,
        mesh=mesh,
        in_specs=(
            P("task", "tensor"),
            P("task", "tensor"),
            P("task", "tensor"),
            P("task", "tensor"),
            P(None, "tensor"),
            P("tensor", None),
            P("task"),
        ),
        out_specs=(P("task", "tensor"), P("tensor", "task")),
        check_vma=False,
    )
```

```python
import functools

import jax
import jax.numpy as jnp
from jax import lax
from jax.experimental import pallas as pl
from jax.experimental.pallas import tpu as pltpu
from jax.sharding import PartitionSpec as P


HD = 128
RATE = 0.25
CORES = 2
PAIRS = 2
CHUNKS = 4
VMEM_LIMIT = 16 * 1024 * 1024


f32 = jnp.float32
bf16 = jnp.bfloat16
Shape = jax.ShapeDtypeStruct


def dot_nn(a, b):
    return lax.dot_general(a, b, (((1,), (0,)), ((), ())), preferred_element_type=f32)


def dot_nt(a, b):
    return lax.dot_general(a, b, (((1,), (1,)), ((), ())), preferred_element_type=f32)


def dot_tn(a, b):
    return lax.dot_general(a, b, (((0,), (0,)), ((), ())), preferred_element_type=f32)


def split_dot(dot, small, big):
    upper = small.astype(bf16)
    lower = (small - upper.astype(f32)).astype(bf16)
    return dot(upper, big) + dot(lower, big)


def by_head(dot, probs_ref, value):
    return jnp.concatenate(
        [dot(probs_ref[h], value[:, h * HD : (h + 1) * HD]) for h in range(probs_ref.shape[0])],
        axis=1,
    )


def call(kernel, out_shape, **kwargs):
    return pl.pallas_call(
        kernel,
        out_shape=out_shape,
        compiler_params=pltpu.CompilerParams(vmem_limit_bytes=VMEM_LIMIT),
        **kwargs,
    )


def whole(array):
    return pl.BlockSpec(array.shape, lambda *unused: (0,) * len(array.shape))


def probs_kernel(split_ref, query_ref, key_ref, out_ref, support_ref, asked_ref):
    heads, length, _ = out_ref.shape
    inside = lax.broadcasted_iota(jnp.int32, (length, 1), 0) < split_ref[0]
    count = split_ref[0].astype(f32)
    support_ref[...] = jnp.where(inside, 1.0, 0.0) / count
    asked_ref[...] = jnp.where(inside, 0.0, 1.0) / (f32(length) - count)
    row = lax.broadcasted_iota(jnp.int32, (length, length), 0)
    col = lax.broadcasted_iota(jnp.int32, (length, length), 1)
    for h in range(heads):
        cols = slice(h * HD, (h + 1) * HD)
        scores = dot_nt(query_ref[:, cols], key_ref[:, cols]) / jnp.sqrt(f32(HD))
        scores = jnp.where(row >= col, scores, f32(-1e30))
        expo = jnp.exp(scores - jnp.max(scores, axis=-1, keepdims=True))
        out_ref[h] = (expo / jnp.sum(expo, axis=-1, keepdims=True)).astype(bf16)


def piece_kernel(place_ref, x_ref, weight_ref, acc_ref, old_ref, out_ref, square_ref):
    @pl.when(pl.program_id(0) == 0)
    def _():
        square_ref[...] = old_ref[...] + row_squares(x_ref[...])

    out_ref[...] = acc_ref[...] + dot_nn(x_ref[...], weight_ref[...])


def row_squares(value):
    value = value.astype(f32)
    return jnp.sum(value * value, axis=-1, keepdims=True)


def first_piece_kernel(place_ref, x_ref, weight_ref, out_ref, square_ref):
    @pl.when(pl.program_id(0) == 0)
    def _():
        square_ref[...] = row_squares(x_ref[...])

    out_ref[...] = dot_nn(x_ref[...], weight_ref[...])


def upper_kernel(wide, place_ref, x_ref, weight_ref, acc_ref, square_ref, probs_ref, upper_ref, mixed_ref, scale_ref, keep_ref):
    @pl.when(pl.program_id(0) == 0)
    def _():
        square = square_ref[...] + row_squares(x_ref[...])
        scale = lax.rsqrt(square / wide + 1e-05)
        keep_ref[...] = scale
        scale_ref[...] = scale

    upper = keep_ref[...] * (acc_ref[...] + dot_nn(x_ref[...], weight_ref[...]))
    upper = upper.astype(bf16)
    upper_ref[...] = upper
    mixed_ref[...] = by_head(dot_nn, probs_ref, upper).astype(bf16)


def gram_kernel(pieces, group_ref, scale_ref, *refs):
    x_refs, (normed_ref, gram_ref) = refs[:pieces], refs[pieces:]
    count, _, step = normed_ref.shape
    span = count // pieces
    scale = scale_ref[...]
    group = group_ref[0]
    gram = None
    for shift in range(pieces):
        normed = (x_refs[shift][...].astype(f32) * scale).astype(bf16)
        term = dot_nt(normed, normed)
        gram = term if gram is None else gram + term
        start = lax.rem(group + pieces - shift, pieces) * span
        for m in range(span):
            normed_ref[start + m] = normed[:, m * step : (m + 1) * step]
    gram_ref[...] = gram


def part_kernel(cross, offset, *refs):
    refs = list(refs)
    take = lambda n: [refs.pop(0) for _ in range(n)]
    left_ref, weight_ref = take(2)
    part = dot_nn(left_ref[...], weight_ref[...])
    if cross is not None:
        cross_ref, error_ref = take(2)
        part = part + cross(cross_ref[...], error_ref[0])
    if offset is not None:
        rows, piece = offset
        group_ref, x_ref, t_ref = take(3)
        gap = x_ref[rows].astype(f32) - t_ref[rows].astype(f32)
        part = part + jnp.where(group_ref[0] == piece, gap, 0.0)
    refs[0][...] = part.astype(bf16)


def finish_kernel(rows, others, matched, merged, chained, filled, tail, n_tail, *refs):
    refs = list(refs)
    take = lambda n: [refs.pop(0) for _ in range(n)]
    part_ref, weight_ref, scale_ref = take(3)
    other_refs = take(others)
    match_in = take(1) if matched else []
    merge_in = take(1) if merged else []
    chain_in = take(2 if matched else 1) if chained else []
    take(1 if filled else 0)
    tail_in = take(n_tail)
    error_ref = take(1)[0]
    if tail is None:
        acc_ref = take(1)[0]
        match_ref = take(1)[0] if matched else None
        tail_out = []
    else:
        n_scratch = 2 if matched else 1
        tail_out = take(len(refs) - n_scratch)
        acc_ref = take(1)[0]
        match_ref = take(1)[0] if matched else None

    total = part_ref[...].astype(f32)
    for other in other_refs:
        total = total + other[...].astype(f32)
    scale = scale_ref[...]
    scaled = scale[rows] * total
    error = scaled.astype(bf16)
    if merged:
        query = merge_in[0][0].astype(f32)
        length, cols = scale.shape[0], query.shape[1]
        gap = jnp.zeros((length - query.shape[0], cols), f32)
        error_ref[0] = jnp.where(
            scale > 0.0, jnp.concatenate([scaled, gap], axis=0), jnp.concatenate([gap, query], axis=0)
        ).astype(bf16)
    else:
        error_ref[0] = error
    acc = dot_nt(error, weight_ref[...])
    match = dot_nt(error, match_in[0][0]) if matched else None
    first = pl.program_id(0) == 0

    @pl.when(first)
    def _():
        acc_ref[...] = acc + chain_in[0][...] if chained else acc
        if matched:
            match_ref[...] = match + chain_in[1][...] if chained else match

    @pl.when(jnp.logical_not(first))
    def _():
        acc_ref[...] += acc
        if matched:
            match_ref[...] += match

    if tail is not None:
        @pl.when(pl.program_id(0) == pl.num_programs(0) - 1)
        def _():
            if matched:
                tail(acc_ref[...], match_ref[...], *tail_in, *tail_out)
            else:
                tail(acc_ref[...], *tail_in, *tail_out)


def step_tail(low, high, acc, probs_ref, gram_ref, upper_ref, mixed_ref, support_ref, next_ref, query_ref, left_ref, cross_ref):
    length, width = upper_ref.shape
    grad_mixed = jnp.concatenate([acc.astype(bf16), jnp.zeros((length - high, width), bf16)], axis=0)
    grad_upper = by_head(dot_tn, probs_ref, grad_mixed).astype(bf16)
    upper = upper_ref[...].astype(f32) - RATE * split_dot(dot_nn, gram_ref[...], grad_upper)
    mixed_next = by_head(dot_nn, probs_ref, upper.astype(bf16)).astype(bf16)
    next_ref[...] = mixed_next
    query_ref[...] = mixed_next[low:]
    mixed = mixed_ref[...]
    inside = support_ref[...] > 0.0
    left_ref[...] = jnp.where(inside, mixed.astype(f32), mixed_next.astype(f32)).astype(bf16)
    cross_ref[...] = (-RATE * dot_nt(mixed_next[low:], mixed[:high])).astype(bf16)


def second_tail(low, high, acc, match, probs_ref, gram_ref, mixed_ref, next_ref, tangent_ref, grad_ref):
    length, width = mixed_ref.shape
    match = -RATE * match
    grad_next = acc + split_dot(dot_nn, match, mixed_ref[:high])
    grad_next = jnp.concatenate([jnp.zeros((low, width), f32), grad_next], axis=0)
    grad_upper = by_head(dot_tn, probs_ref, grad_next.astype(bf16)).astype(bf16)
    upper_dot = -RATE * split_dot(dot_nn, gram_ref[...], grad_upper)
    tangent = by_head(dot_nn, probs_ref, upper_dot.astype(bf16)).astype(bf16)
    tangent_ref[...] = tangent[:high]
    back = split_dot(dot_tn, match, next_ref[low:])
    back = jnp.concatenate([back, jnp.zeros((length - high, width), f32)], axis=0)
    grad_ref[...] = grad_next + back


def third_tail(high, acc, grad_ref, probs_ref, out_ref):
    length, width = grad_ref.shape
    extra = jnp.concatenate([acc, jnp.zeros((length - high, width), f32)], axis=0)
    out_ref[...] = by_head(dot_tn, probs_ref, (grad_ref[...] + extra).astype(bf16)).astype(bf16)


def sources(task, members):
    pairs, cores = PAIRS, CORES
    planes = members // pairs
    plane, pair, core = task // (cores * pairs), lax.rem(task // cores, pairs), lax.rem(task, cores)
    found = [
        lax.rem(plane + planes - turn, planes) * pairs + lax.rem(pair + flip, pairs)
        for flip in range(pairs)
        for turn in range(planes)
    ]
    return found, core


def value_kernel(count, task_ref, cols_ref, *refs):
    blocks, (own_ref, sent_ref) = refs[:count], refs[count:]
    rows = blocks[0].shape[0]
    found, core = sources(task_ref[0], count)
    total = None
    for slot in range(count):
        start = pl.multiple_of(found[slot] * rows, rows)
        term = dot_tn(cols_ref[pl.ds(start, rows), :], blocks[slot][...])
        total = term if total is None else total + term
    half = total.shape[0] // CORES
    top, bottom = total[:half], total[half:]
    own_ref[...] = jnp.where(core == 0, top, bottom)
    sent_ref[...] = jnp.where(core == 0, bottom, top).astype(bf16)


def output_kernel(count, task_ref, merged_ref, error_ref, *refs):
    left, tangent, (own_ref, sent_ref) = refs[:count], refs[count : 2 * count], refs[2 * count :]
    rows, short = left[0].shape[0], tangent[0].shape[0]
    found, core = sources(task_ref[0], count)
    total = None
    for slot in range(count):
        start = pl.multiple_of(found[slot] * rows, rows)
        short_start = pl.multiple_of(found[slot] * short, short)
        term = dot_tn(left[slot][...], merged_ref[pl.ds(start, rows), :])
        term = term + dot_tn(tangent[slot][...], error_ref[pl.ds(short_start, short), :])
        total = term if total is None else total + term
    half = total.shape[1] // CORES
    first, second = total[:, :half], total[:, half:]
    own_ref[...] = jnp.where(core == 0, first, second)
    sent_ref[...] = jnp.where(core == 0, second, first).astype(bf16)


def program(n_task, n_tensor, inputs, targets, queries, key_rows, value_weight, output_weight, splits):
    length, part_width = inputs.shape
    wide = part_width * n_tensor
    heads = queries.shape[1] // HD
    width = heads * HD
    low, high = length // 4, length - length // 4
    lane = wide // CHUNKS
    group = lax.axis_index("tensor").astype(jnp.int32)
    here = group.reshape(1)
    task = lax.axis_index("task").astype(jnp.int32).reshape(1)
    cores, pairs = CORES, PAIRS
    smem = pl.BlockSpec(memory_space=pltpu.SMEM)
    vmem = pl.BlockSpec(memory_space=pltpu.VMEM)
    planes = n_task // (cores * pairs)
    members = planes * pairs

    def over_tensor(value, shift):
        return lax.ppermute(value, "tensor", [(i, (i + shift) % n_tensor) for i in range(n_tensor)])

    def from_others(value):
        return [over_tensor(value, shift) for shift in range(1, n_tensor)]

    def over_task(value, target):
        return lax.ppermute(value, "task", [(i, target(i)) for i in range(n_task)])

    def gathered(value):
        blocks = [value]
        for turn in range(1, planes):
            blocks.append(
                over_task(value, lambda i, turn=turn: (i + turn * cores * pairs) % n_task)
            )
        crossed = [over_task(value, lambda i: i ^ cores)]
        crossed += [over_task(b, lambda i: i ^ cores) for b in blocks[1:]]
        return blocks + crossed

    def spread(value):
        groups = [[m * cores + c for m in range(members)] for c in range(cores)]
        moved = lax.all_to_all(value, "task", split_axis=0, concat_axis=0, axis_index_groups=groups, tiled=True)
        return moved.reshape(members * value.shape[1], value.shape[2])

    x_pieces = [inputs] + from_others(inputs)
    places = [((group - s) % n_tensor).astype(jnp.int32).reshape(1) for s in range(n_tensor)]
    probs, support_weight, query_weight = call(
        probs_kernel,
        [Shape((heads, length, length), bf16), Shape((length, 1), f32), Shape((length, 1), f32)],
        in_specs=[smem, vmem, vmem],
    )(splits, queries, key_rows)

    block = 2 * HD if heads % 2 == 0 else HD
    x_spec = pl.BlockSpec((length, part_width), lambda i, place: (0, 0))
    w_spec = pl.BlockSpec((part_width, block), lambda i, place: (place[0], i))
    cols_spec = pl.BlockSpec((length, block), lambda i, place: (0, i))
    one_spec = pl.BlockSpec((length, 1), lambda i, place: (0, 0))

    def spec(ins, outs, scratch=()):
        return pltpu.PrefetchScalarGridSpec(
            num_scalar_prefetch=1, grid=(width // block,), in_specs=ins, out_specs=outs, scratch_shapes=scratch
        )

    sums = [Shape((length, width), f32), Shape((length, 1), f32)]
    acc, square = call(first_piece_kernel, sums, grid_spec=spec([x_spec, w_spec], [cols_spec, one_spec]))(
        places[0], inputs, value_weight
    )
    for s in range(1, n_tensor - 1):
        acc, square = call(
            piece_kernel, sums, grid_spec=spec([x_spec, w_spec, cols_spec, one_spec], [cols_spec, one_spec])
        )(places[s], x_pieces[s], value_weight, acc, square)
    probs_spec = pl.BlockSpec((block // HD, length, length), lambda i, place: (i, 0, 0))
    upper, mixed, scale = call(
        functools.partial(upper_kernel, wide),
        [Shape((length, width), bf16), Shape((length, width), bf16), Shape((length, 1), f32)],
        grid_spec=spec(
            [x_spec, w_spec, cols_spec, one_spec, probs_spec],
            [cols_spec, cols_spec, one_spec],
            [pltpu.VMEM((length, 1), f32)],
        ),
    )(places[-1], x_pieces[-1], value_weight, acc, square, probs)

    step = wide // members
    steps = lane // step
    normed, gram = call(
        functools.partial(gram_kernel, n_tensor),
        [Shape((members, length, step), bf16), Shape((length, length), f32)],
        in_specs=[smem] + [vmem] * (1 + n_tensor),
    )(here, scale, *x_pieces)
    normed_cols = spread(normed)

    def part_of(c, left, rows, cross=None, pair_of=None, error=None, offset=None):
        ins = [pl.BlockSpec((rows, width), lambda i: (0, 0)), pl.BlockSpec((width, step), lambda i: (0, c * steps + i))]
        args = [left, output_weight]
        if cross is not None:
            ins += [whole(pair_of), pl.BlockSpec((1, error.shape[1], step), lambda i: (c * steps + i, 0, 0))]
            args += [pair_of, error]
        if offset is not None:
            piece, start = c * lane // part_width, c * lane % part_width // step
            offset = (offset, piece)
            ins += [smem] + [pl.BlockSpec((length, step), lambda i: (0, start + i))] * 2
            args += [here, inputs, targets]
        part = call(
            functools.partial(part_kernel, cross, offset),
            Shape((rows, lane), bf16),
            grid=(steps,),
            in_specs=ins,
            out_specs=pl.BlockSpec((rows, step), lambda i: (0, i)),
        )(*args)
        return part, from_others(part)

    def combine(parts, row_slice, weight, matches, merged, tail, tail_args, tail_shapes):
        rows = row_slice.stop - row_slice.start
        errors = None
        chain = []
        for c, (part, others) in enumerate(parts):
            last = c == CHUNKS - 1
            cols = pl.BlockSpec((rows, step), lambda i: (0, i))
            stack = lambda r, c=c: pl.BlockSpec((1, r, step), lambda i: (c * steps + i, 0, 0))
            ins = [cols, pl.BlockSpec((width, step), lambda i, c=c: (0, c * steps + i)), whole(weight)]
            args = [part, output_weight, weight]
            ins += [cols] * len(others)
            args += others
            for extra in (matches, merged):
                if extra is not None:
                    ins.append(stack(extra.shape[1]))
                    args.append(extra)
            ins += [whole(a) for a in chain]
            args += chain
            aliases = {}
            if errors is not None:
                aliases = {len(args): 0}
                ins.append(pl.BlockSpec(memory_space=pl.ANY))
                args.append(errors)
            sums = [Shape((rows, width), f32)] + ([Shape((rows, matches.shape[1]), f32)] if matches is not None else [])
            out_rows = rows if merged is None else length
            outs = [Shape((members, out_rows, step), bf16)]
            out_specs = [stack(out_rows)]
            scratch = []
            n_tail = 0
            if last:
                ins += [whole(a) for a in tail_args]
                args += tail_args
                n_tail = len(tail_args)
                outs += tail_shapes
                out_specs += [whole(s) for s in tail_shapes]
                scratch = [pltpu.VMEM(s.shape, s.dtype) for s in sums]
            else:
                outs += sums
                out_specs += [whole(s) for s in sums]
            results = call(
                functools.partial(
                    finish_kernel, row_slice, len(others), matches is not None, merged is not None,
                    bool(chain), errors is not None, tail if last else None, n_tail,
                ),
                outs,
                grid=(steps,),
                in_specs=ins,
                out_specs=out_specs,
                scratch_shapes=scratch,
                input_output_aliases=aliases,
            )(*args)
            errors = results[0]
            chain = list(results[1:])
        return errors, chain

    parts = [part_of(c, mixed, high, offset=slice(0, high)) for c in range(CHUNKS)]
    error_0, (mixed_next, next_q, left, cross) = combine(
        parts, slice(0, high), support_weight, None, None,
        functools.partial(step_tail, low, high),
        [probs, gram, upper, mixed, support_weight],
        [
            Shape((length, width), bf16),
            Shape((length - low, width), bf16),
            Shape((length, width), bf16),
            Shape((length - low, high), bf16),
        ],
    )
    error_0_cols = spread(error_0)

    parts = [part_of(c, next_q, length - low, dot_nn, cross, error_0, slice(low, length)) for c in range(CHUNKS)]
    left_all = gathered(left)
    error_q, (tangent, grad_rest) = combine(
        parts, slice(low, length), query_weight, error_0, None,
        functools.partial(second_tail, low, high),
        [probs, gram, mixed, mixed_next],
        [Shape((high, width), bf16), Shape((length, width), f32)],
    )
    parts = [part_of(c, tangent, high, dot_tn, cross, error_q) for c in range(CHUNKS)]
    tangent_all = gathered(tangent)
    merged, (right,) = combine(
        parts, slice(0, high), support_weight, None, error_q,
        functools.partial(third_tail, high),
        [grad_rest, probs],
        [Shape((length, width), bf16)],
    )
    right_all = gathered(right)
    merged_cols = spread(merged)

    wide_block = wide // n_task
    own_v, sent_v = call(
        functools.partial(value_kernel, members),
        [Shape((wide_block, width), f32), Shape((wide_block, width), bf16)],
        in_specs=[smem] + [vmem] * (1 + members),
        out_specs=[vmem, vmem],
    )(task, normed_cols, *right_all)
    own_o, sent_o = call(
        functools.partial(output_kernel, members),
        [Shape((width, wide_block), f32), Shape((width, wide_block), bf16)],
        in_specs=[smem] + [vmem] * (2 + 2 * members),
        out_specs=[vmem, vmem],
    )(task, merged_cols, error_0_cols, *left_all, *tangent_all)
    total_value = own_v + over_task(sent_v, lambda i: i ^ 1).astype(f32)
    total_output = own_o + over_task(sent_o, lambda i: i ^ 1).astype(f32)
    return (total_value, total_output)


def solution(mesh):
    body = functools.partial(program, mesh.shape["task"], mesh.shape["tensor"])
    return jax.shard_map(
        body,
        mesh=mesh,
        in_specs=(
            P("task", "tensor"),
            P("task", "tensor"),
            P("task", "tensor"),
            P("task", "tensor"),
            P(None, "tensor"),
            P("tensor", None),
            P("task"),
        ),
        out_specs=(P("task", "tensor"), P("tensor", "task")),
        check_vma=False,
    )
```

```python
import functools

import jax
import jax.numpy as jnp
from jax import lax
from jax.experimental import pallas as pl
from jax.experimental.pallas import tpu as pltpu
from jax.sharding import PartitionSpec as P


HD = 128
RATE = 0.25
CORES = 2
PAIRS = 2
SHARES = (4, 4)
CHUNKS = len(SHARES)
VMEM_LIMIT = 16 * 1024 * 1024


f32 = jnp.float32
bf16 = jnp.bfloat16
Shape = jax.ShapeDtypeStruct


def dot_nn(a, b):
    return lax.dot_general(a, b, (((1,), (0,)), ((), ())), preferred_element_type=f32)


def dot_nt(a, b):
    return lax.dot_general(a, b, (((1,), (1,)), ((), ())), preferred_element_type=f32)


def dot_tn(a, b):
    return lax.dot_general(a, b, (((0,), (0,)), ((), ())), preferred_element_type=f32)


def split_dot(dot, small, big):
    upper = small.astype(bf16)
    lower = (small - upper.astype(f32)).astype(bf16)
    return dot(upper, big) + dot(lower, big)


def by_head(dot, probs_ref, value):
    return jnp.concatenate(
        [dot(probs_ref[h], value[:, h * HD : (h + 1) * HD]) for h in range(probs_ref.shape[0])],
        axis=1,
    )


def call(kernel, out_shape, **kwargs):
    return pl.pallas_call(
        kernel,
        out_shape=out_shape,
        compiler_params=pltpu.CompilerParams(vmem_limit_bytes=VMEM_LIMIT),
        **kwargs,
    )


def whole(array):
    return pl.BlockSpec(array.shape, lambda *unused: (0,) * len(array.shape))


def probs_kernel(split_ref, query_ref, key_ref, out_ref, support_ref, asked_ref):
    heads, length, _ = out_ref.shape
    inside = lax.broadcasted_iota(jnp.int32, (length, 1), 0) < split_ref[0]
    count = split_ref[0].astype(f32)
    support_ref[...] = jnp.where(inside, 1.0, 0.0) / count
    asked_ref[...] = jnp.where(inside, 0.0, 1.0) / (f32(length) - count)
    row = lax.broadcasted_iota(jnp.int32, (length, length), 0)
    col = lax.broadcasted_iota(jnp.int32, (length, length), 1)
    for h in range(heads):
        cols = slice(h * HD, (h + 1) * HD)
        scores = dot_nt(query_ref[:, cols], key_ref[:, cols]) / jnp.sqrt(f32(HD))
        scores = jnp.where(row >= col, scores, f32(-1e30))
        expo = jnp.exp(scores - jnp.max(scores, axis=-1, keepdims=True))
        out_ref[h] = (expo / jnp.sum(expo, axis=-1, keepdims=True)).astype(bf16)


def piece_kernel(place_ref, x_ref, weight_ref, acc_ref, old_ref, out_ref, square_ref):
    @pl.when(pl.program_id(0) == 0)
    def _():
        square_ref[...] = old_ref[...] + row_squares(x_ref[...])

    out_ref[...] = acc_ref[...] + dot_nn(x_ref[...], weight_ref[...])


def copy_kernel(source_ref, out_ref):
    out_ref[...] = source_ref[...]


def place_copy_kernel(place_ref, source_ref, out_ref):
    out_ref[...] = source_ref[...]


def pack_kernel(count, *refs):
    out_ref = refs[-1]
    for turn in range(count):
        first, second = refs[turn], refs[count + turn]
        rows = first.shape[1]
        for flip in range(PAIRS):
            out_ref[turn * PAIRS + flip, :rows] = first[flip]
            out_ref[turn * PAIRS + flip, rows:] = second[flip]


def row_squares(value):
    value = value.astype(f32)
    return jnp.sum(value * value, axis=-1, keepdims=True)


def first_piece_kernel(place_ref, x_ref, weight_ref, out_ref, square_ref):
    @pl.when(pl.program_id(0) == 0)
    def _():
        square_ref[...] = row_squares(x_ref[...])

    out_ref[...] = dot_nn(x_ref[...], weight_ref[...])


def upper_kernel(wide, place_ref, x_ref, weight_ref, acc_ref, square_ref, probs_ref, upper_ref, mixed_ref, scale_ref, keep_ref):
    @pl.when(pl.program_id(0) == 0)
    def _():
        square = square_ref[...] + row_squares(x_ref[...])
        scale = lax.rsqrt(square / wide + 1e-05)
        keep_ref[...] = scale
        scale_ref[...] = scale

    upper = keep_ref[...] * (acc_ref[...] + dot_nn(x_ref[...], weight_ref[...]))
    upper = upper.astype(bf16)
    upper_ref[...] = upper
    mixed_ref[...] = by_head(dot_nn, probs_ref, upper).astype(bf16)


def own_rows(value, group, parts):
    rows = value.shape[0] // parts
    out = value[:rows]
    for p in range(1, parts):
        out = jnp.where(group == p, value[p * rows : (p + 1) * rows], out)
    return out


def all_rows(pieces, group):
    parts = len(pieces)
    if parts == 1:
        return pieces[0]
    out = []
    for p in range(parts):
        piece = pieces[0]
        for shift in range(1, parts):
            piece = jnp.where(lax.rem(group + parts - shift, parts) == p, pieces[shift], piece)
        out.append(piece)
    return jnp.concatenate(out, axis=0)


def deal(ids_ref, parts, blocks_ref, keep_ref, give_ref):
    planes = keep_ref.shape[0]
    group, plane, pair = ids_ref[0], ids_ref[1], ids_ref[2]
    for turn in range(planes):
        base = lax.rem(plane + turn, planes) * PAIRS
        keep_ref[turn] = own_rows(blocks_ref[base + pair], group, parts)
        give_ref[turn] = own_rows(blocks_ref[base + PAIRS - 1 - pair], group, parts)


def deal_kernel(parts, ids_ref, blocks_ref, keep_ref, give_ref):
    deal(ids_ref, parts, blocks_ref, keep_ref, give_ref)


def pair_kernel(keep_ref, take_ref, *out_refs):
    for turn, out_ref in enumerate(out_refs):
        out_ref[0] = keep_ref[turn]
        out_ref[1] = take_ref[turn]


def gram_kernel(pieces, ids_ref, scale_ref, *refs):
    x_refs, (keep_ref, give_ref, gram_ref, blocks_ref) = refs[:pieces], refs[pieces:]
    count, _, step = blocks_ref.shape
    span = count // pieces
    scale = scale_ref[...]
    gram = None
    for shift in range(pieces):
        normed = (x_refs[shift][...].astype(f32) * scale).astype(bf16)
        term = dot_nt(normed, normed)
        gram = term if gram is None else gram + term
        start = lax.rem(ids_ref[0] + pieces - shift, pieces) * span
        for m in range(span):
            blocks_ref[start + m] = normed[:, m * step : (m + 1) * step]
    gram_ref[...] = gram
    deal(ids_ref, pieces, blocks_ref, keep_ref, give_ref)


def part_kernel(cross, offset, *refs):
    refs = list(refs)
    take = lambda n: [refs.pop(0) for _ in range(n)]
    left_ref, weight_ref = take(2)
    part = dot_nn(left_ref[...], weight_ref[...])
    if cross is not None:
        cross_ref, error_ref = take(2)
        part = part + cross(cross_ref[...], error_ref[0])
    if offset is not None:
        rows, begin, span = offset
        piece = (begin + pl.program_id(0)) // span
        group_ref, x_ref, t_ref = take(3)
        gap = x_ref[rows].astype(f32) - t_ref[rows].astype(f32)
        part = part + jnp.where(group_ref[0] == piece, gap, 0.0)
    refs[0][...] = part.astype(bf16)


def finish_kernel(rows, others, matched, merged, chained, filled, tail, n_tail, *refs):
    refs = list(refs)
    take = lambda n: [refs.pop(0) for _ in range(n)]
    part_ref, weight_ref, scale_ref = take(3)
    other_refs = take(others)
    match_in = take(1) if matched else []
    merge_in, (ids_ref,) = (take(1), take(1)) if merged else ([], [None])
    chain_in = take(2 if matched else 1) if chained else []
    take(1 if filled else 0)
    tail_in = take(n_tail)
    error_ref = take(1)[0]
    if tail is None:
        acc_ref = take(1)[0]
        match_ref = take(1)[0] if matched else None
        tail_out = []
    else:
        n_scratch = 2 if matched else 1
        tail_out = take(len(refs) - n_scratch)
        acc_ref = take(1)[0]
        match_ref = take(1)[0] if matched else None

    total = part_ref[...].astype(f32)
    for other in other_refs:
        total = total + other[...].astype(f32)
    scale = scale_ref[...]
    scaled = scale[rows] * total
    error = scaled.astype(bf16)
    if merged:
        query = merge_in[0][0].astype(f32)
        length, cols = scale.shape[0], query.shape[1]
        gap = jnp.zeros((length - query.shape[0], cols), f32)
        both = jnp.where(
            scale > 0.0, jnp.concatenate([scaled, gap], axis=0), jnp.concatenate([gap, query], axis=0)
        )
        error_ref[0] = own_rows(both, ids_ref[0], length // error_ref.shape[1]).astype(bf16)
    else:
        error_ref[0] = error
    acc = dot_nt(error, weight_ref[...])
    match = dot_nt(error, match_in[0][0]) if matched else None
    first = pl.program_id(0) == 0

    @pl.when(first)
    def _():
        acc_ref[...] = acc + chain_in[0][...] if chained else acc
        if matched:
            match_ref[...] = match + chain_in[1][...] if chained else match

    @pl.when(jnp.logical_not(first))
    def _():
        acc_ref[...] += acc
        if matched:
            match_ref[...] += match

    if tail is not None:
        @pl.when(pl.program_id(0) == pl.num_programs(0) - 1)
        def _():
            if matched:
                tail(acc_ref[...], match_ref[...], *tail_in, *tail_out)
            else:
                tail(acc_ref[...], *tail_in, *tail_out)


def step_tail(low, high, acc, probs_ref, gram_ref, upper_ref, mixed_ref, support_ref, next_ref, query_ref, left_ref, cross_ref):
    length, width = upper_ref.shape
    grad_mixed = jnp.concatenate([acc.astype(bf16), jnp.zeros((length - high, width), bf16)], axis=0)
    grad_upper = by_head(dot_tn, probs_ref, grad_mixed).astype(bf16)
    upper = upper_ref[...].astype(f32) - RATE * split_dot(dot_nn, gram_ref[...], grad_upper)
    mixed_next = by_head(dot_nn, probs_ref, upper.astype(bf16)).astype(bf16)
    next_ref[...] = mixed_next
    query_ref[...] = mixed_next[low:]
    mixed = mixed_ref[...]
    inside = support_ref[...] > 0.0
    left_ref[...] = jnp.where(inside, mixed.astype(f32), mixed_next.astype(f32)).astype(bf16)
    cross_ref[...] = (-RATE * dot_nt(mixed_next[low:], mixed[:high])).astype(bf16)


def second_tail(low, high, acc, match, probs_ref, gram_ref, mixed_ref, next_ref, tangent_ref, grad_ref):
    length, width = mixed_ref.shape
    match = -RATE * match
    grad_next = acc + split_dot(dot_nn, match, mixed_ref[:high])
    grad_next = jnp.concatenate([jnp.zeros((low, width), f32), grad_next], axis=0)
    grad_upper = by_head(dot_tn, probs_ref, grad_next.astype(bf16)).astype(bf16)
    upper_dot = -RATE * split_dot(dot_nn, gram_ref[...], grad_upper)
    tangent = by_head(dot_nn, probs_ref, upper_dot.astype(bf16)).astype(bf16)
    tangent_ref[...] = tangent[:high]
    back = split_dot(dot_tn, match, next_ref[low:])
    back = jnp.concatenate([back, jnp.zeros((length - high, width), f32)], axis=0)
    grad_ref[...] = grad_next + back


def third_tail(high, acc, grad_ref, probs_ref, out_ref):
    length, width = grad_ref.shape
    extra = jnp.concatenate([acc, jnp.zeros((length - high, width), f32)], axis=0)
    out_ref[...] = by_head(dot_tn, probs_ref, (grad_ref[...] + extra).astype(bf16)).astype(bf16)


def value_kernel(parts, planes, ids_ref, *refs):
    cols, refs = refs[:parts], refs[parts:]
    blocks, (own_ref, sent_ref) = refs[: planes * PAIRS], refs[planes * PAIRS :]
    group, core = ids_ref[0], ids_ref[3]
    rows = blocks[0].shape[0] // parts
    left = [
        all_rows([c[turn * PAIRS + flip, :rows] for c in cols], group)
        for flip in range(PAIRS)
        for turn in range(planes)
    ]
    total = dot_tn(jnp.concatenate(left, axis=0), jnp.concatenate([b[...] for b in blocks], axis=0))
    half = total.shape[0] // CORES
    top, bottom = total[:half], total[half:]
    own_ref[...] = jnp.where(core == 0, top, bottom)
    sent_ref[...] = jnp.where(core == 0, bottom, top).astype(bf16)


def output_kernel(parts, planes, ids_ref, *refs):
    refs = list(refs)
    take = lambda n: [refs.pop(0) for _ in range(n)]
    count = planes * PAIRS
    merged, cols, left, tangent = take(parts), take(parts), take(count), take(count)
    own_ref, sent_ref = refs
    group, plane, pair, core = [ids_ref[i] for i in range(4)]
    rows = left[0].shape[0] // parts
    right = []
    for flip in range(PAIRS):
        for turn in range(planes):
            source = lax.rem(plane + planes - turn, planes) * PAIRS + lax.rem(pair + flip, PAIRS)
            right.append(all_rows([m[source] for m in merged], group))
    for flip in range(PAIRS):
        for turn in range(planes):
            right.append(all_rows([c[turn * PAIRS + flip, rows:] for c in cols], group))
    total = dot_tn(
        jnp.concatenate([b[...] for b in left + tangent], axis=0), jnp.concatenate(right, axis=0)
    )
    half = total.shape[1] // CORES
    first, second = total[:, :half], total[:, half:]
    own_ref[...] = jnp.where(core == 0, first, second)
    sent_ref[...] = jnp.where(core == 0, second, first).astype(bf16)


def program(n_task, n_tensor, inputs, targets, queries, key_rows, value_weight, output_weight, splits):
    length, part_width = inputs.shape
    wide = part_width * n_tensor
    heads = queries.shape[1] // HD
    width = heads * HD
    low, high = length // 4, length - length // 4
    cores, pairs = CORES, PAIRS
    planes = n_task // (cores * pairs)
    members = planes * pairs
    smem = pl.BlockSpec(memory_space=pltpu.SMEM)
    vmem = pl.BlockSpec(memory_space=pltpu.VMEM)
    group = lax.axis_index("tensor").astype(jnp.int32)
    task = lax.axis_index("task").astype(jnp.int32)
    ids = jnp.stack([group, task // (cores * pairs), (task // cores) % pairs, task % cores])
    places = [((group - s) % n_tensor).astype(jnp.int32).reshape(1) for s in range(n_tensor)]
    inputs, splits, ids, places = lax.optimization_barrier((inputs, splits, ids, places))

    def over_tensor(value, shift):
        return lax.ppermute(value, "tensor", [(i, (i + shift) % n_tensor) for i in range(n_tensor)])

    def from_others(value):
        return [over_tensor(value, shift) for shift in range(1, n_tensor)]

    def over_task(value, target):
        return lax.ppermute(value, "task", [(i, target(i)) for i in range(n_task)])

    def gathered(value):
        blocks = [value]
        for turn in range(1, planes):
            blocks.append(
                over_task(value, lambda i, turn=turn: (i + turn * cores * pairs) % n_task)
            )
        crossed = [over_task(value, lambda i: i ^ cores)]
        crossed += [over_task(b, lambda i: i ^ cores) for b in blocks[1:]]
        return blocks + crossed

    def spread(value):
        groups = [[m * cores + c for m in range(members)] for c in range(cores)]
        moved = lax.all_to_all(value, "task", split_axis=0, concat_axis=0, axis_index_groups=groups, tiled=True)
        return [moved] + from_others(moved)

    def staged(keep, give):
        taken = over_task(give, lambda i: i ^ cores)
        shape = (pairs,) + keep.shape[1:]
        sent = call(pair_kernel, [Shape(shape, bf16)] * planes)(keep, taken)
        got = [sent[0]]
        for turn in range(1, planes):
            got.append(over_task(sent[turn], lambda i, turn=turn: (i + turn * cores * pairs) % n_task))
        return got

    x_pieces = [inputs] + from_others(inputs)
    probs, support_weight, query_weight = call(
        probs_kernel,
        [Shape((heads, length, length), bf16), Shape((length, 1), f32), Shape((length, 1), f32)],
        in_specs=[smem, vmem, vmem],
    )(splits, queries, key_rows)

    block = 2 * HD if heads % 2 == 0 else HD
    x_spec = pl.BlockSpec((length, part_width), lambda i, place: (0, 0))
    w_spec = pl.BlockSpec((part_width, block), lambda i, place: (place[0], i))
    cols_spec = pl.BlockSpec((length, block), lambda i, place: (0, i))
    one_spec = pl.BlockSpec((length, 1), lambda i, place: (0, 0))

    def spec(ins, outs, scratch=()):
        return pltpu.PrefetchScalarGridSpec(
            num_scalar_prefetch=1, grid=(width // block,), in_specs=ins, out_specs=outs, scratch_shapes=scratch
        )

    sums = [Shape((length, width), f32), Shape((length, 1), f32)]
    if n_tensor > 1:
        last_weight = call(
            place_copy_kernel, Shape((part_width, width), bf16),
            grid_spec=spec([w_spec], pl.BlockSpec((part_width, block), lambda i, place: (0, i))),
        )(places[-1], value_weight)
    else:
        last_weight = value_weight
    out_block = 4 * HD
    output_weight = call(
        copy_kernel, Shape((width, wide), bf16), grid=(wide // out_block,),
        in_specs=[pl.BlockSpec((width, out_block), lambda i: (0, i))],
        out_specs=pl.BlockSpec((width, out_block), lambda i: (0, i)),
    )(output_weight)
    acc, square = call(first_piece_kernel, sums, grid_spec=spec([x_spec, w_spec], [cols_spec, one_spec]))(
        places[0], inputs, value_weight
    )
    for s in range(1, n_tensor - 1):
        acc, square = call(
            piece_kernel, sums, grid_spec=spec([x_spec, w_spec, cols_spec, one_spec], [cols_spec, one_spec])
        )(places[s], x_pieces[s], value_weight, acc, square)
    probs_spec = pl.BlockSpec((block // HD, length, length), lambda i, place: (i, 0, 0))
    upper, mixed, scale = call(
        functools.partial(upper_kernel, wide),
        [Shape((length, width), bf16), Shape((length, width), bf16), Shape((length, 1), f32)],
        grid_spec=spec(
            [x_spec, pl.BlockSpec((part_width, block), lambda i, place: (0, i)), cols_spec, one_spec, probs_spec],
            [cols_spec, cols_spec, one_spec],
            [pltpu.VMEM((length, 1), f32)],
        ),
    )(places[-1], x_pieces[-1], last_weight, acc, square, probs)

    step = wide // members
    shares = [share * members // sum(SHARES) for share in SHARES]
    starts = [sum(shares[:c]) for c in range(CHUNKS)]
    span = part_width // step
    dealt = Shape((planes, length // n_tensor, step), bf16)
    keep, give, gram = call(
        functools.partial(gram_kernel, n_tensor),
        [dealt, dealt, Shape((length, length), f32)],
        in_specs=[smem] + [vmem] * (1 + n_tensor),
        scratch_shapes=[pltpu.VMEM((members, length, step), bf16)],
    )(ids, scale, *x_pieces)
    normed_cols = staged(keep, give)

    def part_of(c, left, rows, cross=None, pair_of=None, error=None, offset=None):
        begin = starts[c]
        ins = [pl.BlockSpec((rows, width), lambda i: (0, 0)), pl.BlockSpec((width, step), lambda i: (0, begin + i))]
        args = [left, output_weight]
        if cross is not None:
            ins += [whole(pair_of), pl.BlockSpec((1, error.shape[1], step), lambda i: (begin + i, 0, 0))]
            args += [pair_of, error]
        if offset is not None:
            offset = (offset, begin, span)
            ins += [smem] + [pl.BlockSpec((length, step), lambda i: (0, (begin + i) % span))] * 2
            args += [ids, inputs, targets]
        part = call(
            functools.partial(part_kernel, cross, offset),
            Shape((rows, shares[c] * step), bf16),
            grid=(shares[c],),
            in_specs=ins,
            out_specs=pl.BlockSpec((rows, step), lambda i: (0, i)),
        )(*args)
        return part, from_others(part)

    def combine(parts, row_slice, weight, matches, merged, tail, tail_args, tail_shapes):
        rows = row_slice.stop - row_slice.start
        errors = None
        chain = []
        for c, (part, others) in enumerate(parts):
            last = c == CHUNKS - 1
            cols = pl.BlockSpec((rows, step), lambda i: (0, i))
            stack = lambda r, c=c: pl.BlockSpec((1, r, step), lambda i: (starts[c] + i, 0, 0))
            ins = [cols, pl.BlockSpec((width, step), lambda i, c=c: (0, starts[c] + i)), whole(weight)]
            args = [part, output_weight, weight]
            ins += [cols] * len(others)
            args += others
            for extra in (matches, merged):
                if extra is not None:
                    ins.append(stack(extra.shape[1]))
                    args.append(extra)
            if merged is not None:
                ins.append(smem)
                args.append(ids)
            ins += [whole(a) for a in chain]
            args += chain
            aliases = {}
            if errors is not None:
                aliases = {len(args): 0}
                ins.append(pl.BlockSpec(memory_space=pl.ANY))
                args.append(errors)
            sums = [Shape((rows, width), f32)] + ([Shape((rows, matches.shape[1]), f32)] if matches is not None else [])
            out_rows = rows if merged is None else length // n_tensor
            outs = [Shape((members, out_rows, step), bf16)]
            out_specs = [stack(out_rows)]
            scratch = []
            n_tail = 0
            if last:
                ins += [whole(a) for a in tail_args]
                args += tail_args
                n_tail = len(tail_args)
                outs += tail_shapes
                out_specs += [whole(s) for s in tail_shapes]
                scratch = [pltpu.VMEM(s.shape, s.dtype) for s in sums]
            else:
                outs += sums
                out_specs += [whole(s) for s in sums]
            results = call(
                functools.partial(
                    finish_kernel, row_slice, len(others), matches is not None, merged is not None,
                    bool(chain), errors is not None, tail if last else None, n_tail,
                ),
                outs,
                grid=(shares[c],),
                in_specs=ins,
                out_specs=out_specs,
                scratch_shapes=scratch,
                input_output_aliases=aliases,
            )(*args)
            errors = results[0]
            chain = list(results[1:])
        return errors, chain

    parts = [part_of(c, mixed, high, offset=slice(0, high)) for c in range(CHUNKS)]
    error_0, (mixed_next, next_q, left, cross) = combine(
        parts, slice(0, high), support_weight, None, None,
        functools.partial(step_tail, low, high),
        [probs, gram, upper, mixed, support_weight],
        [
            Shape((length, width), bf16),
            Shape((length - low, width), bf16),
            Shape((length, width), bf16),
            Shape((length - low, high), bf16),
        ],
    )
    dealt = Shape((planes, high // n_tensor, step), bf16)
    keep, give = call(
        functools.partial(deal_kernel, n_tensor), [dealt, dealt], in_specs=[smem, vmem]
    )(ids, error_0)
    error_0_cols = staged(keep, give)

    parts = [part_of(c, next_q, length - low, dot_nn, cross, error_0, slice(low, length)) for c in range(CHUNKS)]
    left_all = gathered(left)
    error_q, (tangent, grad_rest) = combine(
        parts, slice(low, length), query_weight, error_0, None,
        functools.partial(second_tail, low, high),
        [probs, gram, mixed, mixed_next],
        [Shape((high, width), bf16), Shape((length, width), f32)],
    )
    parts = [part_of(c, tangent, high, dot_tn, cross, error_q) for c in range(CHUNKS)]
    tangent_all = gathered(tangent)
    merged, (right,) = combine(
        parts, slice(0, high), support_weight, None, error_q,
        functools.partial(third_tail, high),
        [grad_rest, probs],
        [Shape((length, width), bf16)],
    )
    right_all = gathered(right)
    merged_cols = spread(merged)

    kept = call(
        functools.partial(pack_kernel, planes), Shape((members, (length + high) // n_tensor, step), bf16)
    )(*normed_cols, *error_0_cols)
    packed = [kept] + from_others(kept)

    wide_block = wide // n_task
    own_v, sent_v = call(
        functools.partial(value_kernel, n_tensor, planes),
        [Shape((wide_block, width), f32), Shape((wide_block, width), bf16)],
        in_specs=[smem] + [vmem] * (n_tensor + members),
        out_specs=[vmem, vmem],
    )(ids, *packed, *right_all)
    own_o, sent_o = call(
        functools.partial(output_kernel, n_tensor, planes),
        [Shape((width, wide_block), f32), Shape((width, wide_block), bf16)],
        in_specs=[smem] + [vmem] * (2 * n_tensor + 2 * members),
        out_specs=[vmem, vmem],
    )(ids, *merged_cols, *packed, *left_all, *tangent_all)
    total_value = own_v + over_task(sent_v, lambda i: i ^ 1).astype(f32)
    total_output = own_o + over_task(sent_o, lambda i: i ^ 1).astype(f32)
    return (total_value, total_output)


def solution(mesh):
    body = functools.partial(program, mesh.shape["task"], mesh.shape["tensor"])
    return jax.shard_map(
        body,
        mesh=mesh,
        in_specs=(
            P("task", "tensor"),
            P("task", "tensor"),
            P("task", "tensor"),
            P("task", "tensor"),
            P(None, "tensor"),
            P("tensor", None),
            P("task"),
        ),
        out_specs=(P("task", "tensor"), P("tensor", "task")),
        check_vma=False,
    )
```

```python
import functools

import jax
import jax.numpy as jnp
from jax import lax
from jax.experimental import pallas as pl
from jax.experimental.pallas import tpu as pltpu
from jax.sharding import PartitionSpec as P


HD = 128
RATE = 0.25
CORES = 2
TASK, TENSOR = "task", "tensor"
PAIRS = 2
SHARES = (2, 3, 3)
CHUNKS = len(SHARES)
VMEM_LIMIT = 16 * 1024 * 1024


f32 = jnp.float32
bf16 = jnp.bfloat16
Shape = jax.ShapeDtypeStruct


def dot_nn(a, b):
    return lax.dot_general(a, b, (((1,), (0,)), ((), ())), preferred_element_type=f32)


def dot_nt(a, b):
    return lax.dot_general(a, b, (((1,), (1,)), ((), ())), preferred_element_type=f32)


def dot_tn(a, b):
    return lax.dot_general(a, b, (((0,), (0,)), ((), ())), preferred_element_type=f32)


def split_dot(dot, small, big):
    upper = small.astype(bf16)
    lower = (small - upper.astype(f32)).astype(bf16)
    return dot(upper, big) + dot(lower, big)


def by_head(dot, probs_ref, value):
    return jnp.concatenate(
        [dot(probs_ref[h], value[:, h * HD : (h + 1) * HD]) for h in range(probs_ref.shape[0])],
        axis=1,
    )


def call(kernel, out_shape, **kwargs):
    return pl.pallas_call(
        kernel,
        out_shape=out_shape,
        compiler_params=pltpu.CompilerParams(vmem_limit_bytes=VMEM_LIMIT),
        **kwargs,
    )


def whole(array):
    return pl.BlockSpec(array.shape, lambda *unused: (0,) * len(array.shape))


def probs_kernel(split_ref, query_ref, key_ref, out_ref, support_ref, asked_ref):
    heads, length, _ = out_ref.shape
    inside = lax.broadcasted_iota(jnp.int32, (length, 1), 0) < split_ref[0]
    count = split_ref[0].astype(f32)
    support_ref[...] = jnp.where(inside, 1.0, 0.0) / count
    asked_ref[...] = jnp.where(inside, 0.0, 1.0) / (f32(length) - count)
    row = lax.broadcasted_iota(jnp.int32, (length, length), 0)
    col = lax.broadcasted_iota(jnp.int32, (length, length), 1)
    for h in range(heads):
        cols = slice(h * HD, (h + 1) * HD)
        scores = dot_nt(query_ref[:, cols], key_ref[:, cols]) / jnp.sqrt(f32(HD))
        scores = jnp.where(row >= col, scores, f32(-1e30))
        expo = jnp.exp(scores - jnp.max(scores, axis=-1, keepdims=True))
        out_ref[h] = (expo / jnp.sum(expo, axis=-1, keepdims=True)).astype(bf16)


def piece_kernel(place_ref, x_ref, weight_ref, acc_ref, old_ref, out_ref, square_ref):
    @pl.when(pl.program_id(0) == 0)
    def _():
        square_ref[...] = old_ref[...] + row_squares(x_ref[...])

    out_ref[...] = acc_ref[...] + dot_nn(x_ref[...], weight_ref[...])


def copy_kernel(source_ref, out_ref):
    out_ref[...] = source_ref[...]


def place_copy_kernel(place_ref, source_ref, out_ref):
    out_ref[...] = source_ref[...]


def flips_kernel(*refs):
    out_refs = refs[-PAIRS:]
    for turn, ref in enumerate(refs[:-PAIRS]):
        for flip in range(PAIRS):
            out_refs[flip][turn] = ref[flip]


def sides_kernel(ids_ref, *refs):
    keep_ref, give_ref = refs[-2:]
    pair = ids_ref[2]
    for turn, ref in enumerate(refs[:-2]):
        keep_ref[turn] = ref[pair]
        give_ref[turn] = ref[PAIRS - 1 - pair]


def stack_kernel(count, *refs):
    out_ref = refs[-1]
    for flip in range(PAIRS):
        start = 0
        for piece in refs[flip:-1:PAIRS]:
            rows = piece.shape[1]
            for turn in range(count):
                out_ref[turn * PAIRS + flip, start : start + rows] = piece[turn]
            start += rows


def row_squares(value):
    value = value.astype(f32)
    return jnp.sum(value * value, axis=-1, keepdims=True)


def first_piece_kernel(place_ref, x_ref, weight_ref, out_ref, square_ref):
    @pl.when(pl.program_id(0) == 0)
    def _():
        square_ref[...] = row_squares(x_ref[...])

    out_ref[...] = dot_nn(x_ref[...], weight_ref[...])


def upper_kernel(wide, place_ref, x_ref, weight_ref, acc_ref, square_ref, probs_ref, upper_ref, mixed_ref, scale_ref, keep_ref):
    @pl.when(pl.program_id(0) == 0)
    def _():
        square = square_ref[...] + row_squares(x_ref[...])
        scale = lax.rsqrt(square / wide + 1e-05)
        keep_ref[...] = scale
        scale_ref[...] = scale

    upper = keep_ref[...] * (acc_ref[...] + dot_nn(x_ref[...], weight_ref[...]))
    upper = upper.astype(bf16)
    upper_ref[...] = upper
    mixed_ref[...] = by_head(dot_nn, probs_ref, upper).astype(bf16)


def own_rows(value, group, parts):
    rows = value.shape[0] // parts
    out = value[:rows]
    for p in range(1, parts):
        out = jnp.where(group == p, value[p * rows : (p + 1) * rows], out)
    return out


def all_rows(pieces, group):
    parts = len(pieces)
    if parts == 1:
        return pieces[0]
    out = []
    for p in range(parts):
        piece = pieces[0]
        for shift in range(1, parts):
            piece = jnp.where(lax.rem(group + parts - shift, parts) == p, pieces[shift], piece)
        out.append(piece)
    return jnp.concatenate(out, axis=0)


def deal(ids_ref, parts, blocks_ref, keep_ref, give_ref):
    planes = keep_ref.shape[0]
    group, plane, pair = ids_ref[0], ids_ref[1], ids_ref[2]
    for turn in range(planes):
        base = lax.rem(plane + turn, planes) * PAIRS
        keep_ref[turn] = own_rows(blocks_ref[base + pair], group, parts)
        give_ref[turn] = own_rows(blocks_ref[base + PAIRS - 1 - pair], group, parts)


def deal_kernel(parts, ids_ref, blocks_ref, *out_refs):
    planes = len(out_refs)
    group, plane = ids_ref[0], ids_ref[1]
    for turn, out_ref in enumerate(out_refs):
        base = lax.rem(plane + turn, planes) * PAIRS
        for flip in range(PAIRS):
            out_ref[flip] = own_rows(blocks_ref[base + flip], group, parts)


def pair_kernel(keep_ref, take_ref, *out_refs):
    for turn, out_ref in enumerate(out_refs):
        out_ref[0] = keep_ref[turn]
        out_ref[1] = take_ref[turn]


def gram_kernel(pieces, ids_ref, scale_ref, *refs):
    x_refs, (keep_ref, give_ref, gram_ref, blocks_ref) = refs[:pieces], refs[pieces:]
    count, _, step = blocks_ref.shape
    span = count // pieces
    scale = scale_ref[...]
    gram = None
    for shift in range(pieces):
        normed = (x_refs[shift][...].astype(f32) * scale).astype(bf16)
        term = dot_nt(normed, normed)
        gram = term if gram is None else gram + term
        start = lax.rem(ids_ref[0] + pieces - shift, pieces) * span
        for m in range(span):
            blocks_ref[start + m] = normed[:, m * step : (m + 1) * step]
    gram_ref[...] = gram
    deal(ids_ref, pieces, blocks_ref, keep_ref, give_ref)


def part_kernel(cross, offset, *refs):
    refs = list(refs)
    take = lambda n: [refs.pop(0) for _ in range(n)]
    left_ref, weight_ref = take(2)
    part = dot_nn(left_ref[...], weight_ref[...])
    if cross is not None:
        cross_ref, error_ref = take(2)
        part = part + cross(cross_ref[...], error_ref[0])
    if offset is not None:
        rows, begin, span = offset
        piece = (begin + pl.program_id(0)) // span
        group_ref, x_ref, t_ref = take(3)
        gap = x_ref[rows].astype(f32) - t_ref[rows].astype(f32)
        part = part + jnp.where(group_ref[0] == piece, gap, 0.0)
    refs[0][...] = part.astype(bf16)


def finish_kernel(rows, others, matched, merged, chained, filled, tail, n_tail, *refs):
    refs = list(refs)
    take = lambda n: [refs.pop(0) for _ in range(n)]
    part_ref, weight_ref, scale_ref = take(3)
    other_refs = take(others)
    match_in = take(1) if matched else []
    merge_in = take(1) if merged else []
    chain_in = take(2 if matched else 1) if chained else []
    take(1 if filled else 0)
    tail_in = take(n_tail)
    error_ref = take(1)[0]
    if tail is None:
        acc_ref = take(1)[0]
        match_ref = take(1)[0] if matched else None
        tail_out = []
    else:
        n_scratch = 2 if matched else 1
        tail_out = take(len(refs) - n_scratch)
        acc_ref = take(1)[0]
        match_ref = take(1)[0] if matched else None

    total = part_ref[...].astype(f32)
    for other in other_refs:
        total = total + other[...].astype(f32)
    scale = scale_ref[...]
    scaled = scale[rows] * total
    error = scaled.astype(bf16)
    if merged:
        query = merge_in[0][0].astype(f32)
        length, cols = scale.shape[0], query.shape[1]
        gap = jnp.zeros((length - query.shape[0], cols), f32)
        both = jnp.where(
            scale > 0.0, jnp.concatenate([scaled, gap], axis=0), jnp.concatenate([gap, query], axis=0)
        )
        error_ref[0] = both.astype(bf16)
    else:
        error_ref[0] = error
    acc = dot_nt(error, weight_ref[...])
    match = dot_nt(error, match_in[0][0]) if matched else None
    first = pl.program_id(0) == 0

    @pl.when(first)
    def _():
        acc_ref[...] = acc + chain_in[0][...] if chained else acc
        if matched:
            match_ref[...] = match + chain_in[1][...] if chained else match

    @pl.when(jnp.logical_not(first))
    def _():
        acc_ref[...] += acc
        if matched:
            match_ref[...] += match

    if tail is not None:
        @pl.when(pl.program_id(0) == pl.num_programs(0) - 1)
        def _():
            if matched:
                tail(acc_ref[...], match_ref[...], *tail_in, *tail_out)
            else:
                tail(acc_ref[...], *tail_in, *tail_out)


def step_tail(low, high, acc, probs_ref, gram_ref, upper_ref, mixed_ref, support_ref, next_ref, query_ref, left_ref, cross_ref):
    length, width = upper_ref.shape
    grad_mixed = jnp.concatenate([acc.astype(bf16), jnp.zeros((length - high, width), bf16)], axis=0)
    grad_upper = by_head(dot_tn, probs_ref, grad_mixed).astype(bf16)
    upper = upper_ref[...].astype(f32) - RATE * split_dot(dot_nn, gram_ref[...], grad_upper)
    mixed_next = by_head(dot_nn, probs_ref, upper.astype(bf16)).astype(bf16)
    next_ref[...] = mixed_next
    query_ref[...] = mixed_next[low:]
    mixed = mixed_ref[...]
    inside = support_ref[...] > 0.0
    left_ref[...] = jnp.where(inside, mixed.astype(f32), mixed_next.astype(f32)).astype(bf16)
    cross_ref[...] = (-RATE * dot_nt(mixed_next[low:], mixed[:high])).astype(bf16)


def second_tail(low, high, acc, match, probs_ref, gram_ref, mixed_ref, next_ref, tangent_ref, grad_ref):
    length, width = mixed_ref.shape
    match = -RATE * match
    grad_next = acc + split_dot(dot_nn, match, mixed_ref[:high])
    grad_next = jnp.concatenate([jnp.zeros((low, width), f32), grad_next], axis=0)
    grad_upper = by_head(dot_tn, probs_ref, grad_next.astype(bf16)).astype(bf16)
    upper_dot = -RATE * split_dot(dot_nn, gram_ref[...], grad_upper)
    tangent = by_head(dot_nn, probs_ref, upper_dot.astype(bf16)).astype(bf16)
    tangent_ref[...] = tangent[:high]
    back = split_dot(dot_tn, match, next_ref[low:])
    back = jnp.concatenate([back, jnp.zeros((length - high, width), f32)], axis=0)
    grad_ref[...] = grad_next + back


def third_tail(high, acc, grad_ref, probs_ref, out_ref):
    length, width = grad_ref.shape
    extra = jnp.concatenate([acc, jnp.zeros((length - high, width), f32)], axis=0)
    out_ref[...] = by_head(dot_tn, probs_ref, (grad_ref[...] + extra).astype(bf16)).astype(bf16)


def value_kernel(parts, planes, ids_ref, *refs):
    cols, refs = refs[:parts], refs[parts:]
    blocks, (own_ref, sent_ref) = refs[: planes * PAIRS], refs[planes * PAIRS :]
    group, core = ids_ref[0], ids_ref[3]
    left = [
        all_rows([c[turn * PAIRS + flip] for c in cols], group) for flip in range(PAIRS) for turn in range(planes)
    ]
    total = dot_tn(jnp.concatenate(left, axis=0), jnp.concatenate([b[...] for b in blocks], axis=0))
    half = total.shape[0] // CORES
    top, bottom = total[:half], total[half:]
    own_ref[...] = jnp.where(core == 0, top, bottom)
    sent_ref[...] = jnp.where(core == 0, bottom, top).astype(bf16)


def output_kernel(parts, planes, ids_ref, *refs):
    refs = list(refs)
    take = lambda n: [refs.pop(0) for _ in range(n)]
    count = planes * PAIRS
    merged, error, left, tangent = take(PAIRS * parts), take(parts), take(count), take(count)
    own_ref, sent_ref = refs
    group, core = ids_ref[0], ids_ref[3]
    slots = [(turn, flip) for flip in range(PAIRS) for turn in range(planes)]
    right = [all_rows([merged[flip * parts + p][turn] for p in range(parts)], group) for turn, flip in slots]
    right += [all_rows([e[turn * PAIRS + flip] for e in error], group) for turn, flip in slots]
    total = dot_tn(
        jnp.concatenate([b[...] for b in left + tangent], axis=0), jnp.concatenate(right, axis=0)
    )
    half = total.shape[1] // CORES
    first, second = total[:, :half], total[:, half:]
    own_ref[...] = jnp.where(core == 0, first, second)
    sent_ref[...] = jnp.where(core == 0, second, first).astype(bf16)


def program(n_task, n_tensor, inputs, targets, queries, key_rows, value_weight, output_weight, splits):
    length, part_width = inputs.shape
    wide = part_width * n_tensor
    heads = queries.shape[1] // HD
    width = heads * HD
    low, high = length // 4, length - length // 4
    cores, pairs = CORES, PAIRS
    planes = n_task // (cores * pairs)
    members = planes * pairs
    smem = pl.BlockSpec(memory_space=pltpu.SMEM)
    vmem = pl.BlockSpec(memory_space=pltpu.VMEM)
    group = lax.axis_index(TENSOR).astype(jnp.int32)
    task = lax.axis_index(TASK).astype(jnp.int32)
    ids = jnp.stack([group, task // (cores * pairs), (task // cores) % pairs, task % cores])
    places = [((group - s) % n_tensor).astype(jnp.int32).reshape(1) for s in range(n_tensor)]
    inputs, splits, ids, places = lax.optimization_barrier((inputs, splits, ids, places))

    def over_tensor(value, shift):
        return lax.ppermute(value, TENSOR, [(i, (i + shift) % n_tensor) for i in range(n_tensor)])

    def from_others(value):
        return [over_tensor(value, shift) for shift in range(1, n_tensor)]

    def over_task(value, target):
        return lax.ppermute(value, TASK, [(i, target(i)) for i in range(n_task)])

    def turned(value, turn):
        return over_task(value, lambda i: (i + turn * cores * pairs) % n_task)

    def ring(value, both_ways):
        blocks, rounds = [value] + [None] * (planes - 1), [0] * planes
        reach = planes // 2 if both_ways else planes - 1
        for turn in range(1, reach + 1):
            rounds[turn] = min(turn, 3)
            blocks[turn] = turned(blocks[turn - 1], 1)
        for turn in range(planes - 1, reach, -1):
            rounds[turn] = min(planes - turn, 3)
            blocks[turn] = turned(blocks[(turn + 1) % planes], planes - 1)
        crossed = []
        for turn in range(planes):
            crossed.append(over_task(blocks[turn], lambda i: i ^ cores))
        return blocks + crossed

    def dealt_out(blocks):
        shape = Shape((pairs, blocks.shape[1] // n_tensor, blocks.shape[2]), bf16)
        sent = call(
            functools.partial(deal_kernel, n_tensor), [shape] * planes, in_specs=[smem, vmem]
        )(ids, blocks)
        return [sent[0]] + [turned(sent[turn], turn) for turn in range(1, planes)]

    def sides(got):
        shape = Shape((planes,) + got[0].shape[1:], bf16)
        keep, give = call(sides_kernel, [shape] * 2, in_specs=[smem] + [vmem] * planes)(ids, *got)
        return keep, over_task(give, lambda i: i ^ cores)

    def stacked(flips):
        shape = Shape((members,) + flips[0].shape[1:], bf16)
        kept = call(functools.partial(stack_kernel, planes), shape)(*flips)
        return [kept] + from_others(kept)

    def staged(keep, give):
        taken = over_task(give, lambda i: i ^ cores)
        shape = (pairs,) + keep.shape[1:]
        sent = call(pair_kernel, [Shape(shape, bf16)] * planes)(keep, taken)
        return [sent[0]] + [turned(sent[turn], turn) for turn in range(1, planes)]

    x_pieces = [inputs] + from_others(inputs)
    probs, support_weight, query_weight = call(
        probs_kernel,
        [Shape((heads, length, length), bf16), Shape((length, 1), f32), Shape((length, 1), f32)],
        in_specs=[smem, vmem, vmem],
    )(splits, queries, key_rows)

    block = 2 * HD if heads % 2 == 0 else HD
    x_spec = pl.BlockSpec((length, part_width), lambda i, place: (0, 0))
    w_spec = pl.BlockSpec((part_width, block), lambda i, place: (place[0], i))
    cols_spec = pl.BlockSpec((length, block), lambda i, place: (0, i))
    one_spec = pl.BlockSpec((length, 1), lambda i, place: (0, 0))

    def spec(ins, outs, scratch=()):
        return pltpu.PrefetchScalarGridSpec(
            num_scalar_prefetch=1, grid=(width // block,), in_specs=ins, out_specs=outs, scratch_shapes=scratch
        )

    sums = [Shape((length, width), f32), Shape((length, 1), f32)]
    if n_tensor > 1:
        last_weight = call(
            place_copy_kernel, Shape((part_width, width), bf16),
            grid_spec=spec([w_spec], pl.BlockSpec((part_width, block), lambda i, place: (0, i))),
        )(places[-1], value_weight)
    else:
        last_weight = value_weight
    out_block = 4 * HD
    output_weight = call(
        copy_kernel, Shape((width, wide), bf16), grid=(wide // out_block,),
        in_specs=[pl.BlockSpec((width, out_block), lambda i: (0, i))],
        out_specs=pl.BlockSpec((width, out_block), lambda i: (0, i)),
    )(output_weight)
    acc, square = call(first_piece_kernel, sums, grid_spec=spec([x_spec, w_spec], [cols_spec, one_spec]))(
        places[0], inputs, value_weight
    )
    for s in range(1, n_tensor - 1):
        acc, square = call(
            piece_kernel, sums, grid_spec=spec([x_spec, w_spec, cols_spec, one_spec], [cols_spec, one_spec])
        )(places[s], x_pieces[s], value_weight, acc, square)
    probs_spec = pl.BlockSpec((block // HD, length, length), lambda i, place: (i, 0, 0))
    upper, mixed, scale = call(
        functools.partial(upper_kernel, wide),
        [Shape((length, width), bf16), Shape((length, width), bf16), Shape((length, 1), f32)],
        grid_spec=spec(
            [x_spec, pl.BlockSpec((part_width, block), lambda i, place: (0, i)), cols_spec, one_spec, probs_spec],
            [cols_spec, cols_spec, one_spec],
            [pltpu.VMEM((length, 1), f32)],
        ),
    )(places[-1], x_pieces[-1], last_weight, acc, square, probs)

    step = wide // members
    shares = [share * members // sum(SHARES) for share in SHARES]
    starts = [sum(shares[:c]) for c in range(CHUNKS)]
    span = part_width // step
    dealt = Shape((planes, length // n_tensor, step), bf16)
    keep, give, gram = call(
        functools.partial(gram_kernel, n_tensor),
        [dealt, dealt, Shape((length, length), f32)],
        in_specs=[smem] + [vmem] * (1 + n_tensor),
        scratch_shapes=[pltpu.VMEM((members, length, step), bf16)],
    )(ids, scale, *x_pieces)
    got = staged(keep, give)
    flips = call(flips_kernel, [Shape((planes,) + got[0].shape[1:], bf16)] * pairs)(*got)
    normed_cols = stacked(flips)

    def part_of(c, left, rows, cross=None, pair_of=None, error=None, offset=None):
        begin = starts[c]
        ins = [pl.BlockSpec((rows, width), lambda i: (0, 0)), pl.BlockSpec((width, step), lambda i: (0, begin + i))]
        args = [left, output_weight]
        if cross is not None:
            ins += [whole(pair_of), pl.BlockSpec((1, error.shape[1], step), lambda i: (begin + i, 0, 0))]
            args += [pair_of, error]
        if offset is not None:
            offset = (offset, begin, span)
            ins += [smem] + [pl.BlockSpec((length, step), lambda i: (0, (begin + i) % span))] * 2
            args += [ids, inputs, targets]
        part = call(
            functools.partial(part_kernel, cross, offset),
            Shape((rows, shares[c] * step), bf16),
            grid=(shares[c],),
            in_specs=ins,
            out_specs=pl.BlockSpec((rows, step), lambda i: (0, i)),
        )(*args)
        return part, from_others(part)

    def combine(parts, row_slice, weight, matches, merged, tail, tail_args, tail_shapes):
        rows = row_slice.stop - row_slice.start
        errors = None
        chain = []
        for c, (part, others) in enumerate(parts):
            last = c == CHUNKS - 1
            cols = pl.BlockSpec((rows, step), lambda i: (0, i))
            stack = lambda r, c=c: pl.BlockSpec((1, r, step), lambda i: (starts[c] + i, 0, 0))
            ins = [cols, pl.BlockSpec((width, step), lambda i, c=c: (0, starts[c] + i)), whole(weight)]
            args = [part, output_weight, weight]
            ins += [cols] * len(others)
            args += others
            for extra in (matches, merged):
                if extra is not None:
                    ins.append(stack(extra.shape[1]))
                    args.append(extra)
            ins += [whole(a) for a in chain]
            args += chain
            aliases = {}
            if errors is not None:
                aliases = {len(args): 0}
                ins.append(pl.BlockSpec(memory_space=pl.ANY))
                args.append(errors)
            sums = [Shape((rows, width), f32)] + ([Shape((rows, matches.shape[1]), f32)] if matches is not None else [])
            out_rows = rows if merged is None else length
            outs = [Shape((members, out_rows, step), bf16)]
            out_specs = [stack(out_rows)]
            scratch = []
            n_tail = 0
            if last:
                ins += [whole(a) for a in tail_args]
                args += tail_args
                n_tail = len(tail_args)
                outs += tail_shapes
                out_specs += [whole(s) for s in tail_shapes]
                scratch = [pltpu.VMEM(s.shape, s.dtype) for s in sums]
            else:
                outs += sums
                out_specs += [whole(s) for s in sums]
            results = call(
                functools.partial(
                    finish_kernel, row_slice, len(others), matches is not None, merged is not None,
                    bool(chain), errors is not None, tail if last else None, n_tail,
                ),
                outs,
                grid=(shares[c],),
                in_specs=ins,
                out_specs=out_specs,
                scratch_shapes=scratch,
                input_output_aliases=aliases,
            )(*args)
            errors = results[0]
            chain = list(results[1:])
        return errors, chain

    parts = [part_of(c, mixed, high, offset=slice(0, high)) for c in range(CHUNKS)]
    error_0, (mixed_next, next_q, left, cross) = combine(
        parts, slice(0, high), support_weight, None, None,
        functools.partial(step_tail, low, high),
        [probs, gram, upper, mixed, support_weight],
        [
            Shape((length, width), bf16),
            Shape((length - low, width), bf16),
            Shape((length, width), bf16),
            Shape((length - low, high), bf16),
        ],
    )
    error_0_cols = stacked(sides(dealt_out(error_0)))

    parts = [part_of(c, next_q, length - low, dot_nn, cross, error_0, slice(low, length)) for c in range(CHUNKS)]
    left_all = ring(left, False)
    error_q, (tangent, grad_rest) = combine(
        parts, slice(low, length), query_weight, error_0, None,
        functools.partial(second_tail, low, high),
        [probs, gram, mixed, mixed_next],
        [Shape((high, width), bf16), Shape((length, width), f32)],
    )
    parts = [part_of(c, tangent, high, dot_tn, cross, error_q) for c in range(CHUNKS)]
    tangent_all = ring(tangent, False)
    merged, (right,) = combine(
        parts, slice(0, high), support_weight, None, error_q,
        functools.partial(third_tail, high),
        [grad_rest, probs],
        [Shape((length, width), bf16)],
    )
    right_all = ring(right, True)
    merged_cols = []
    for part in sides(dealt_out(merged)):
        merged_cols += [part] + from_others(part)

    wide_block = wide // n_task
    own_v, sent_v = call(
        functools.partial(value_kernel, n_tensor, planes),
        [Shape((wide_block, width), f32), Shape((wide_block, width), bf16)],
        in_specs=[smem] + [vmem] * (n_tensor + members),
        out_specs=[vmem, vmem],
    )(ids, *normed_cols, *right_all)
    total_value = own_v + over_task(sent_v, lambda i: i ^ 1).astype(f32)
    own_o, sent_o = call(
        functools.partial(output_kernel, n_tensor, planes),
        [Shape((width, wide_block), f32), Shape((width, wide_block), bf16)],
        in_specs=[smem] + [vmem] * ((1 + pairs) * n_tensor + 2 * members),
        out_specs=[vmem, vmem],
    )(ids, *merged_cols, *error_0_cols, *left_all, *tangent_all)
    total_output = own_o + over_task(sent_o, lambda i: i ^ 1).astype(f32)
    return (total_value, total_output)


def solution(mesh):
    body = functools.partial(program, mesh.shape[TASK], mesh.shape[TENSOR])
    return jax.shard_map(
        body,
        mesh=mesh,
        in_specs=(
            P(TASK, TENSOR),
            P(TASK, TENSOR),
            P(TASK, TENSOR),
            P(TASK, TENSOR),
            P(None, TENSOR),
            P(TENSOR, None),
            P(TASK),
        ),
        out_specs=(P(TASK, TENSOR), P(TENSOR, TASK)),
        check_vma=False,
    )
```

```python
import functools

import jax
import jax.numpy as jnp
from jax import lax
from jax.experimental import pallas as pl
from jax.experimental.pallas import tpu as pltpu
from jax.sharding import PartitionSpec as P


HD = 128
RATE = 0.25
CORES = 2
TASK, TENSOR = "task", "tensor"
PAIRS = 2
SHARES = (2, 3, 3)
CHUNKS = len(SHARES)
VMEM_LIMIT = 16 * 1024 * 1024


f32 = jnp.float32
bf16 = jnp.bfloat16
Shape = jax.ShapeDtypeStruct


def dot_nn(a, b):
    return lax.dot_general(a, b, (((1,), (0,)), ((), ())), preferred_element_type=f32)


def dot_nt(a, b):
    return lax.dot_general(a, b, (((1,), (1,)), ((), ())), preferred_element_type=f32)


def dot_tn(a, b):
    return lax.dot_general(a, b, (((0,), (0,)), ((), ())), preferred_element_type=f32)


def split_dot(dot, small, big):
    upper = small.astype(bf16)
    lower = (small - upper.astype(f32)).astype(bf16)
    return dot(upper, big) + dot(lower, big)


def by_head(dot, probs_ref, value):
    return jnp.concatenate(
        [dot(probs_ref[h], value[:, h * HD : (h + 1) * HD]) for h in range(probs_ref.shape[0])],
        axis=1,
    )


def call(kernel, out_shape, **kwargs):
    return pl.pallas_call(
        kernel,
        out_shape=out_shape,
        compiler_params=pltpu.CompilerParams(vmem_limit_bytes=VMEM_LIMIT),
        **kwargs,
    )


def whole(array):
    return pl.BlockSpec(array.shape, lambda *unused: (0,) * len(array.shape))


def probs_kernel(split_ref, query_ref, key_ref, out_ref, support_ref, asked_ref):
    heads, length, _ = out_ref.shape
    inside = lax.broadcasted_iota(jnp.int32, (length, 1), 0) < split_ref[0]
    count = split_ref[0].astype(f32)
    support_ref[...] = jnp.where(inside, 1.0, 0.0) / count
    asked_ref[...] = jnp.where(inside, 0.0, 1.0) / (f32(length) - count)
    row = lax.broadcasted_iota(jnp.int32, (length, length), 0)
    col = lax.broadcasted_iota(jnp.int32, (length, length), 1)
    for h in range(heads):
        cols = slice(h * HD, (h + 1) * HD)
        scores = dot_nt(query_ref[:, cols], key_ref[:, cols]) / jnp.sqrt(f32(HD))
        scores = jnp.where(row >= col, scores, f32(-1e30))
        expo = jnp.exp(scores - jnp.max(scores, axis=-1, keepdims=True))
        out_ref[h] = (expo / jnp.sum(expo, axis=-1, keepdims=True)).astype(bf16)


def piece_kernel(place_ref, x_ref, weight_ref, acc_ref, old_ref, out_ref, square_ref):
    @pl.when(pl.program_id(0) == 0)
    def _():
        square_ref[...] = old_ref[...] + row_squares(x_ref[...])

    out_ref[...] = acc_ref[...] + dot_nn(x_ref[...], weight_ref[...])


def copy_kernel(source_ref, out_ref):
    out_ref[...] = source_ref[...]


def place_copy_kernel(place_ref, source_ref, out_ref):
    out_ref[...] = source_ref[...]


def flips_kernel(*refs):
    out_refs = refs[-PAIRS:]
    for turn, ref in enumerate(refs[:-PAIRS]):
        for flip in range(PAIRS):
            out_refs[flip][turn] = ref[flip]


def sides_kernel(ids_ref, *refs):
    keep_ref, give_ref = refs[-2:]
    pair = ids_ref[2]
    for turn, ref in enumerate(refs[:-2]):
        keep_ref[turn] = ref[pair]
        give_ref[turn] = ref[PAIRS - 1 - pair]


def stack_kernel(count, *refs):
    out_ref = refs[-1]
    for flip in range(PAIRS):
        start = 0
        for piece in refs[flip:-1:PAIRS]:
            rows = piece.shape[1]
            for turn in range(count):
                out_ref[turn * PAIRS + flip, start : start + rows] = piece[turn]
            start += rows


def row_squares(value):
    value = value.astype(f32)
    return jnp.sum(value * value, axis=-1, keepdims=True)


def first_piece_kernel(place_ref, x_ref, weight_ref, out_ref, square_ref):
    @pl.when(pl.program_id(0) == 0)
    def _():
        square_ref[...] = row_squares(x_ref[...])

    out_ref[...] = dot_nn(x_ref[...], weight_ref[...])


def upper_kernel(wide, place_ref, x_ref, weight_ref, acc_ref, square_ref, probs_ref, upper_ref, mixed_ref, scale_ref, keep_ref):
    @pl.when(pl.program_id(0) == 0)
    def _():
        square = square_ref[...] + row_squares(x_ref[...])
        scale = lax.rsqrt(square / wide + 1e-05)
        keep_ref[...] = scale
        scale_ref[...] = scale

    upper = keep_ref[...] * (acc_ref[...] + dot_nn(x_ref[...], block_of(weight_ref, 0, upper_ref.shape[1])))
    upper = upper.astype(bf16)
    upper_ref[...] = upper
    mixed_ref[...] = by_head(dot_nn, probs_ref, upper).astype(bf16)


def own_rows(value, group, parts):
    rows = value.shape[0] // parts
    out = value[:rows]
    for p in range(1, parts):
        out = jnp.where(group == p, value[p * rows : (p + 1) * rows], out)
    return out


def all_rows(pieces, group):
    parts = len(pieces)
    if parts == 1:
        return pieces[0]
    out = []
    for p in range(parts):
        piece = pieces[0]
        for shift in range(1, parts):
            piece = jnp.where(lax.rem(group + parts - shift, parts) == p, pieces[shift], piece)
        out.append(piece)
    return jnp.concatenate(out, axis=0)


def deal(ids_ref, parts, blocks_ref, keep_ref, give_ref):
    planes = keep_ref.shape[0]
    group, plane, pair = ids_ref[0], ids_ref[1], ids_ref[2]
    for turn in range(planes):
        base = lax.rem(plane + turn, planes) * PAIRS
        keep_ref[turn] = own_rows(blocks_ref[base + pair], group, parts)
        give_ref[turn] = own_rows(blocks_ref[base + PAIRS - 1 - pair], group, parts)


def deal_kernel(parts, ids_ref, blocks_ref, *out_refs):
    planes = len(out_refs)
    group, plane = ids_ref[0], ids_ref[1]
    for turn, out_ref in enumerate(out_refs):
        base = lax.rem(plane + turn, planes) * PAIRS
        for flip in range(PAIRS):
            out_ref[flip] = own_rows(blocks_ref[base + flip], group, parts)


def pair_kernel(keep_ref, take_ref, *out_refs):
    for turn, out_ref in enumerate(out_refs):
        out_ref[0] = keep_ref[turn]
        out_ref[1] = take_ref[turn]


def gram_kernel(pieces, ids_ref, scale_ref, *refs):
    x_refs, (keep_ref, give_ref, gram_ref, blocks_ref) = refs[:pieces], refs[pieces:]
    count, _, step = blocks_ref.shape
    span = count // pieces
    scale = scale_ref[...]
    gram = None
    for shift in range(pieces):
        normed = (x_refs[shift][...].astype(f32) * scale).astype(bf16)
        term = dot_nt(normed, normed)
        gram = term if gram is None else gram + term
        start = lax.rem(ids_ref[0] + pieces - shift, pieces) * span
        for m in range(span):
            blocks_ref[start + m] = normed[:, m * step : (m + 1) * step]
    gram_ref[...] = gram
    deal(ids_ref, pieces, blocks_ref, keep_ref, give_ref)


def block_of(weight_ref, begin, step):
    start = pl.multiple_of((begin + pl.program_id(0)) * step, step)
    return weight_ref[:, pl.ds(start, step)]


def part_kernel(begin, cross, offset, *refs):
    refs = list(refs)
    take = lambda n: [refs.pop(0) for _ in range(n)]
    left_ref, weight_ref = take(2)
    part = dot_nn(left_ref[...], block_of(weight_ref, begin, refs[-1].shape[1]))
    if cross is not None:
        cross_ref, error_ref = take(2)
        part = part + cross(cross_ref[...], error_ref[0])
    if offset is not None:
        rows, span = offset
        piece = (begin + pl.program_id(0)) // span
        group_ref, x_ref, t_ref = take(3)
        gap = x_ref[rows].astype(f32) - t_ref[rows].astype(f32)
        part = part + jnp.where(group_ref[0] == piece, gap, 0.0)
    refs[0][...] = part.astype(bf16)


def finish_kernel(begin, rows, others, matched, merged, chained, filled, tail, n_tail, *refs):
    refs = list(refs)
    take = lambda n: [refs.pop(0) for _ in range(n)]
    part_ref, weight_ref, scale_ref = take(3)
    other_refs = take(others)
    match_in = take(1) if matched else []
    merge_in = take(1) if merged else []
    chain_in = take(2 if matched else 1) if chained else []
    take(1 if filled else 0)
    tail_in = take(n_tail)
    error_ref = take(1)[0]
    if tail is None:
        acc_ref = take(1)[0]
        match_ref = take(1)[0] if matched else None
        tail_out = []
    else:
        n_scratch = 2 if matched else 1
        tail_out = take(len(refs) - n_scratch)
        acc_ref = take(1)[0]
        match_ref = take(1)[0] if matched else None

    total = part_ref[...].astype(f32)
    for other in other_refs:
        total = total + other[...].astype(f32)
    scale = scale_ref[...]
    scaled = scale[rows] * total
    error = scaled.astype(bf16)
    if merged:
        query = merge_in[0][0].astype(f32)
        length, cols = scale.shape[0], query.shape[1]
        gap = jnp.zeros((length - query.shape[0], cols), f32)
        both = jnp.where(
            scale > 0.0, jnp.concatenate([scaled, gap], axis=0), jnp.concatenate([gap, query], axis=0)
        )
        error_ref[0] = both.astype(bf16)
    else:
        error_ref[0] = error
    acc = dot_nt(error, block_of(weight_ref, begin, error.shape[1]))
    match = dot_nt(error, match_in[0][0]) if matched else None
    first = pl.program_id(0) == 0

    @pl.when(first)
    def _():
        acc_ref[...] = acc + chain_in[0][...] if chained else acc
        if matched:
            match_ref[...] = match + chain_in[1][...] if chained else match

    @pl.when(jnp.logical_not(first))
    def _():
        acc_ref[...] += acc
        if matched:
            match_ref[...] += match

    if tail is not None:
        @pl.when(pl.program_id(0) == pl.num_programs(0) - 1)
        def _():
            if matched:
                tail(acc_ref[...], match_ref[...], *tail_in, *tail_out)
            else:
                tail(acc_ref[...], *tail_in, *tail_out)


def step_tail(low, high, acc, probs_ref, gram_ref, upper_ref, mixed_ref, support_ref, next_ref, query_ref, left_ref, cross_ref):
    length, width = upper_ref.shape
    grad_mixed = jnp.concatenate([acc.astype(bf16), jnp.zeros((length - high, width), bf16)], axis=0)
    grad_upper = by_head(dot_tn, probs_ref, grad_mixed).astype(bf16)
    upper = upper_ref[...].astype(f32) - RATE * split_dot(dot_nn, gram_ref[...], grad_upper)
    mixed_next = by_head(dot_nn, probs_ref, upper.astype(bf16)).astype(bf16)
    next_ref[...] = mixed_next
    query_ref[...] = mixed_next[low:]
    mixed = mixed_ref[...]
    inside = support_ref[...] > 0.0
    left_ref[...] = jnp.where(inside, mixed.astype(f32), mixed_next.astype(f32)).astype(bf16)
    cross_ref[...] = (-RATE * dot_nt(mixed_next[low:], mixed[:high])).astype(bf16)


def second_tail(low, high, acc, match, probs_ref, gram_ref, mixed_ref, next_ref, tangent_ref, grad_ref):
    length, width = mixed_ref.shape
    match = -RATE * match
    grad_next = acc + split_dot(dot_nn, match, mixed_ref[:high])
    grad_next = jnp.concatenate([jnp.zeros((low, width), f32), grad_next], axis=0)
    grad_upper = by_head(dot_tn, probs_ref, grad_next.astype(bf16)).astype(bf16)
    upper_dot = -RATE * split_dot(dot_nn, gram_ref[...], grad_upper)
    tangent = by_head(dot_nn, probs_ref, upper_dot.astype(bf16)).astype(bf16)
    tangent_ref[...] = tangent[:high]
    back = split_dot(dot_tn, match, next_ref[low:])
    back = jnp.concatenate([back, jnp.zeros((length - high, width), f32)], axis=0)
    grad_ref[...] = grad_next + back


def third_tail(high, acc, grad_ref, probs_ref, out_ref):
    length, width = grad_ref.shape
    extra = jnp.concatenate([acc, jnp.zeros((length - high, width), f32)], axis=0)
    out_ref[...] = by_head(dot_tn, probs_ref, (grad_ref[...] + extra).astype(bf16)).astype(bf16)


def value_kernel(parts, planes, ids_ref, *refs):
    cols, refs = refs[:parts], refs[parts:]
    blocks, (own_ref, sent_ref) = refs[: planes * PAIRS], refs[planes * PAIRS :]
    group, core = ids_ref[0], ids_ref[3]
    left = [
        all_rows([c[turn * PAIRS + flip] for c in cols], group) for flip in range(PAIRS) for turn in range(planes)
    ]
    total = dot_tn(jnp.concatenate(left, axis=0), jnp.concatenate([b[...] for b in blocks], axis=0))
    half = total.shape[0] // CORES
    top, bottom = total[:half], total[half:]
    own_ref[...] = jnp.where(core == 0, top, bottom)
    sent_ref[...] = jnp.where(core == 0, bottom, top).astype(bf16)


def output_kernel(parts, planes, ids_ref, *refs):
    refs = list(refs)
    take = lambda n: [refs.pop(0) for _ in range(n)]
    count = planes * PAIRS
    merged, error, left, tangent = take(PAIRS * parts), take(parts), take(count), take(count)
    own_ref, sent_ref = refs
    group, core = ids_ref[0], ids_ref[3]
    slots = [(turn, flip) for flip in range(PAIRS) for turn in range(planes)]
    right = [all_rows([merged[flip * parts + p][turn] for p in range(parts)], group) for turn, flip in slots]
    right += [all_rows([e[turn * PAIRS + flip] for e in error], group) for turn, flip in slots]
    total = dot_tn(
        jnp.concatenate([b[...] for b in left + tangent], axis=0), jnp.concatenate(right, axis=0)
    )
    half = total.shape[1] // CORES
    first, second = total[:, :half], total[:, half:]
    own_ref[...] = jnp.where(core == 0, first, second)
    sent_ref[...] = jnp.where(core == 0, second, first).astype(bf16)


def program(n_task, n_tensor, inputs, targets, queries, key_rows, value_weight, output_weight, splits):
    length, part_width = inputs.shape
    wide = part_width * n_tensor
    heads = queries.shape[1] // HD
    width = heads * HD
    low, high = length // 4, length - length // 4
    cores, pairs = CORES, PAIRS
    planes = n_task // (cores * pairs)
    members = planes * pairs
    smem = pl.BlockSpec(memory_space=pltpu.SMEM)
    vmem = pl.BlockSpec(memory_space=pltpu.VMEM)
    group = lax.axis_index(TENSOR).astype(jnp.int32)
    task = lax.axis_index(TASK).astype(jnp.int32)
    ids = jnp.stack([group, task // (cores * pairs), (task // cores) % pairs, task % cores])
    places = [((group - s) % n_tensor).astype(jnp.int32).reshape(1) for s in range(n_tensor)]
    inputs, splits, ids, places = lax.optimization_barrier((inputs, splits, ids, places))

    def over_tensor(value, shift):
        return lax.ppermute(value, TENSOR, [(i, (i + shift) % n_tensor) for i in range(n_tensor)])

    def from_others(value):
        return [over_tensor(value, shift) for shift in range(1, n_tensor)]

    def over_task(value, target):
        return lax.ppermute(value, TASK, [(i, target(i)) for i in range(n_task)])

    def turned(value, turn):
        return over_task(value, lambda i: (i + turn * cores * pairs) % n_task)

    def ring(value, both_ways):
        blocks, rounds = [value] + [None] * (planes - 1), [0] * planes
        reach = planes // 2 if both_ways else planes - 1
        for turn in range(1, reach + 1):
            rounds[turn] = min(turn, 3)
            blocks[turn] = turned(blocks[turn - 1], 1)
        for turn in range(planes - 1, reach, -1):
            rounds[turn] = min(planes - turn, 3)
            blocks[turn] = turned(blocks[(turn + 1) % planes], planes - 1)
        crossed = []
        for turn in range(planes):
            crossed.append(over_task(blocks[turn], lambda i: i ^ cores))
        return blocks + crossed

    def dealt_out(blocks):
        shape = Shape((pairs, blocks.shape[1] // n_tensor, blocks.shape[2]), bf16)
        sent = call(
            functools.partial(deal_kernel, n_tensor), [shape] * planes, in_specs=[smem, vmem]
        )(ids, blocks)
        return [sent[0]] + [turned(sent[turn], turn) for turn in range(1, planes)]

    def sides(got):
        shape = Shape((planes,) + got[0].shape[1:], bf16)
        keep, give = call(sides_kernel, [shape] * 2, in_specs=[smem] + [vmem] * planes)(ids, *got)
        return keep, over_task(give, lambda i: i ^ cores)

    def stacked(flips):
        shape = Shape((members,) + flips[0].shape[1:], bf16)
        kept = call(functools.partial(stack_kernel, planes), shape)(*flips)
        return [kept] + from_others(kept)

    def staged(keep, give):
        taken = over_task(give, lambda i: i ^ cores)
        shape = (pairs,) + keep.shape[1:]
        sent = call(pair_kernel, [Shape(shape, bf16)] * planes)(keep, taken)
        return [sent[0]] + [turned(sent[turn], turn) for turn in range(1, planes)]

    x_pieces = [inputs] + from_others(inputs)
    probs, support_weight, query_weight = call(
        probs_kernel,
        [Shape((heads, length, length), bf16), Shape((length, 1), f32), Shape((length, 1), f32)],
        in_specs=[smem, vmem, vmem],
    )(splits, queries, key_rows)

    block = 2 * HD if heads % 2 == 0 else HD
    x_spec = pl.BlockSpec((length, part_width), lambda i, place: (0, 0))
    w_spec = pl.BlockSpec((part_width, block), lambda i, place: (place[0], i))
    cols_spec = pl.BlockSpec((length, block), lambda i, place: (0, i))
    one_spec = pl.BlockSpec((length, 1), lambda i, place: (0, 0))

    def spec(ins, outs, scratch=()):
        return pltpu.PrefetchScalarGridSpec(
            num_scalar_prefetch=1, grid=(width // block,), in_specs=ins, out_specs=outs, scratch_shapes=scratch
        )

    sums = [Shape((length, width), f32), Shape((length, 1), f32)]
    if n_tensor > 1:
        last_weight = call(
            place_copy_kernel, Shape((part_width, width), bf16),
            grid_spec=spec([w_spec], pl.BlockSpec((part_width, block), lambda i, place: (0, i))),
        )(places[-1], value_weight)
    else:
        last_weight = value_weight
    out_block = 4 * HD
    output_weight = call(
        copy_kernel, Shape((width, wide), bf16), grid=(wide // out_block,),
        in_specs=[pl.BlockSpec((width, out_block), lambda i: (0, i))],
        out_specs=pl.BlockSpec((width, out_block), lambda i: (0, i)),
    )(output_weight)
    acc, square = call(first_piece_kernel, sums, grid_spec=spec([x_spec, w_spec], [cols_spec, one_spec]))(
        places[0], inputs, value_weight
    )
    for s in range(1, n_tensor - 1):
        acc, square = call(
            piece_kernel, sums, grid_spec=spec([x_spec, w_spec, cols_spec, one_spec], [cols_spec, one_spec])
        )(places[s], x_pieces[s], value_weight, acc, square)
    probs_spec = pl.BlockSpec((block // HD, length, length), lambda i, place: (i, 0, 0))
    upper, mixed, scale = call(
        functools.partial(upper_kernel, wide),
        [Shape((length, width), bf16), Shape((length, width), bf16), Shape((length, 1), f32)],
        grid_spec=spec(
            [x_spec, vmem, cols_spec, one_spec, probs_spec],
            [cols_spec, cols_spec, one_spec],
            [pltpu.VMEM((length, 1), f32)],
        ),
    )(places[-1], x_pieces[-1], last_weight, acc, square, probs)

    step = wide // members
    shares = [share * members // sum(SHARES) for share in SHARES]
    starts = [sum(shares[:c]) for c in range(CHUNKS)]
    span = part_width // step
    dealt = Shape((planes, length // n_tensor, step), bf16)
    keep, give, gram = call(
        functools.partial(gram_kernel, n_tensor),
        [dealt, dealt, Shape((length, length), f32)],
        in_specs=[smem] + [vmem] * (1 + n_tensor),
        scratch_shapes=[pltpu.VMEM((members, length, step), bf16)],
    )(ids, scale, *x_pieces)
    got = staged(keep, give)
    flips = call(flips_kernel, [Shape((planes,) + got[0].shape[1:], bf16)] * pairs)(*got)
    normed_cols = stacked(flips)

    def part_of(c, left, rows, cross=None, pair_of=None, error=None, offset=None):
        begin = starts[c]
        ins = [pl.BlockSpec((rows, width), lambda i: (0, 0)), vmem]
        args = [left, output_weight]
        if cross is not None:
            ins += [whole(pair_of), pl.BlockSpec((1, error.shape[1], step), lambda i: (begin + i, 0, 0))]
            args += [pair_of, error]
        if offset is not None:
            offset = (offset, span)
            ins += [smem] + [pl.BlockSpec((length, step), lambda i: (0, (begin + i) % span))] * 2
            args += [ids, inputs, targets]
        part = call(
            functools.partial(part_kernel, begin, cross, offset),
            Shape((rows, shares[c] * step), bf16),
            grid=(shares[c],),
            in_specs=ins,
            out_specs=pl.BlockSpec((rows, step), lambda i: (0, i)),
        )(*args)
        return part, from_others(part)

    def combine(parts, row_slice, weight, matches, merged, tail, tail_args, tail_shapes):
        rows = row_slice.stop - row_slice.start
        errors = None
        chain = []
        for c, (part, others) in enumerate(parts):
            last = c == CHUNKS - 1
            cols = pl.BlockSpec((rows, step), lambda i: (0, i))
            stack = lambda r, c=c: pl.BlockSpec((1, r, step), lambda i: (starts[c] + i, 0, 0))
            ins = [cols, vmem, whole(weight)]
            args = [part, output_weight, weight]
            ins += [cols] * len(others)
            args += others
            for extra in (matches, merged):
                if extra is not None:
                    ins.append(stack(extra.shape[1]))
                    args.append(extra)
            ins += [whole(a) for a in chain]
            args += chain
            aliases = {}
            if errors is not None:
                aliases = {len(args): 0}
                ins.append(pl.BlockSpec(memory_space=pl.ANY))
                args.append(errors)
            sums = [Shape((rows, width), f32)] + ([Shape((rows, matches.shape[1]), f32)] if matches is not None else [])
            out_rows = rows if merged is None else length
            outs = [Shape((members, out_rows, step), bf16)]
            out_specs = [stack(out_rows)]
            scratch = []
            n_tail = 0
            if last:
                ins += [whole(a) for a in tail_args]
                args += tail_args
                n_tail = len(tail_args)
                outs += tail_shapes
                out_specs += [whole(s) for s in tail_shapes]
                scratch = [pltpu.VMEM(s.shape, s.dtype) for s in sums]
            else:
                outs += sums
                out_specs += [whole(s) for s in sums]
            results = call(
                functools.partial(
                    finish_kernel, starts[c], row_slice, len(others), matches is not None, merged is not None,
                    bool(chain), errors is not None, tail if last else None, n_tail,
                ),
                outs,
                grid=(shares[c],),
                in_specs=ins,
                out_specs=out_specs,
                scratch_shapes=scratch,
                input_output_aliases=aliases,
            )(*args)
            errors = results[0]
            chain = list(results[1:])
        return errors, chain

    parts = [part_of(c, mixed, high, offset=slice(0, high)) for c in range(CHUNKS)]
    error_0, (mixed_next, next_q, left, cross) = combine(
        parts, slice(0, high), support_weight, None, None,
        functools.partial(step_tail, low, high),
        [probs, gram, upper, mixed, support_weight],
        [
            Shape((length, width), bf16),
            Shape((length - low, width), bf16),
            Shape((length, width), bf16),
            Shape((length - low, high), bf16),
        ],
    )
    error_0_cols = stacked(sides(dealt_out(error_0)))

    parts = [part_of(c, next_q, length - low, dot_nn, cross, error_0, slice(low, length)) for c in range(CHUNKS)]
    left_all = ring(left, False)
    error_q, (tangent, grad_rest) = combine(
        parts, slice(low, length), query_weight, error_0, None,
        functools.partial(second_tail, low, high),
        [probs, gram, mixed, mixed_next],
        [Shape((high, width), bf16), Shape((length, width), f32)],
    )
    parts = [part_of(c, tangent, high, dot_tn, cross, error_q) for c in range(CHUNKS)]
    tangent_all = ring(tangent, False)
    merged, (right,) = combine(
        parts, slice(0, high), support_weight, None, error_q,
        functools.partial(third_tail, high),
        [grad_rest, probs],
        [Shape((length, width), bf16)],
    )
    right_all = ring(right, True)
    merged_cols = []
    for part in sides(dealt_out(merged)):
        merged_cols += [part] + from_others(part)

    wide_block = wide // n_task
    own_v, sent_v = call(
        functools.partial(value_kernel, n_tensor, planes),
        [Shape((wide_block, width), f32), Shape((wide_block, width), bf16)],
        in_specs=[smem] + [vmem] * (n_tensor + members),
        out_specs=[vmem, vmem],
    )(ids, *normed_cols, *right_all)
    total_value = own_v + over_task(sent_v, lambda i: i ^ 1).astype(f32)
    own_o, sent_o = call(
        functools.partial(output_kernel, n_tensor, planes),
        [Shape((width, wide_block), f32), Shape((width, wide_block), bf16)],
        in_specs=[smem] + [vmem] * ((1 + pairs) * n_tensor + 2 * members),
        out_specs=[vmem, vmem],
    )(ids, *merged_cols, *error_0_cols, *left_all, *tangent_all)
    total_output = own_o + over_task(sent_o, lambda i: i ^ 1).astype(f32)
    return (total_value, total_output)


def solution(mesh):
    body = functools.partial(program, mesh.shape[TASK], mesh.shape[TENSOR])
    return jax.shard_map(
        body,
        mesh=mesh,
        in_specs=(
            P(TASK, TENSOR),
            P(TASK, TENSOR),
            P(TASK, TENSOR),
            P(TASK, TENSOR),
            P(None, TENSOR),
            P(TENSOR, None),
            P(TASK),
        ),
        out_specs=(P(TASK, TENSOR), P(TENSOR, TASK)),
        check_vma=False,
    )
```
